8 devices in a mesh: rep: 1 (over z), dp: 8 (over x, y, core).
Axes of the slice: x: 2, y: 2, z: 1, core: 2. Of those that a mesh axis runs over, the one named last changes fastest.
Arguments:
- x: bfloat16 [8, 2048, 1152], P(('rep', 'dp'))
- dy: bfloat16 [8, 2048, 1152], P(('rep', 'dp'))
- w_gate: bfloat16 [2, 1152, 4608], P(None, 'dp')
- w_up: bfloat16 [2, 1152, 4608], P(None, 'dp')
- w_down: bfloat16 [2, 4608, 1152], P(None, 'dp')
- m_w_gate: float32 [2, 1152, 4608], P(None, 'dp')
- m_w_up: float32 [2, 1152, 4608], P(None, 'dp')
- m_w_down: float32 [2, 4608, 1152], P(None, 'dp')
- v_w_gate: float32 [2, 1152, 4608], P(None, 'dp')
- v_w_up: float32 [2, 1152, 4608], P(None, 'dp')
- v_w_down: float32 [2, 4608, 1152], P(None, 'dp')
Outputs:
- output 1: bfloat16 [2, 1152, 4608], P('rep', 'dp')
- output 2: bfloat16 [2, 1152, 4608], P('rep', 'dp')
- output 3: bfloat16 [2, 4608, 1152], P('rep', 'dp')
- output 4: float32 [2, 1152, 4608], P('rep', 'dp')
- output 5: float32 [2, 1152, 4608], P('rep', 'dp')
- output 6: float32 [2, 4608, 1152], P('rep', 'dp')
- output 7: float32 [2, 1152, 4608], P('rep', 'dp')
- output 8: float32 [2, 1152, 4608], P('rep', 'dp')
- output 9: float32 [2, 4608, 1152], P('rep', 'dp')
All inputs are finite; a program needn't handle non-finite values.
Results may differ from the reference program's by a relative error of at most 0.022.
Values are sent between devices in bfloat16 or wider.
A program may use at most 2 GiB of HBM per device.

```python
import jax
import jax.numpy as jnp
from jax import lax

SEQUENCES = 8
TOKENS = 2048
D = 1152
FF = 4608
LAYERS = 2
NAMES = ("w_gate", "w_up", "w_down")
SHAPES = {"w_gate": (LAYERS, D, FF), "w_up": (LAYERS, D, FF), "w_down": (LAYERS, FF, D)}


def bump(key, n, height):
    away = (jnp.arange(n, dtype=jnp.int32) - jax.random.randint(key, (), 0, n, jnp.int32)) % n
    return jnp.where(away < n // 8, height, 1.0)


def together(key, own, strength):
    shared = jax.random.normal(key, own.shape[1:], jnp.float32)
    return (own + strength * shared) * lax.rsqrt(1 + strength * strength)


def setup_inputs(seed: int = 0, part: int = 0) -> dict:
    kx, kdy, ka, kb, kz, kf, kh, kl, *keys = jax.random.split(jax.random.key(seed), 8 + 3 * len(NAMES))
    kx, kdy, ka, kb = (jax.random.fold_in(k, part) for k in (kx, kdy, ka, kb))
    kw, km, kv = (keys[i::3] for i in range(3))
    shape = (SEQUENCES, TOKENS, D)
    much_x, much_dy = jax.random.uniform(kz, (2,), jnp.float32, 0.0, 1.0)
    loud = 2.0 ** jax.random.uniform(jax.random.fold_in(kz, 1), (), jnp.float32, -1.0, 2.0)
    layers = 2.0 ** jax.random.uniform(kl, (LAYERS, 1, 1), jnp.float32, -1.0, 1.0)
    x = together(ka, jax.random.normal(kx, shape, jnp.float32), much_x) * bump(kf, D, 4.0)
    dy = together(kb, jax.random.normal(kdy, shape, jnp.float32), much_dy)
    drawn = {"x": x.astype(jnp.bfloat16), "dy": (loud * dy * (SEQUENCES * TOKENS) ** -0.5).astype(jnp.bfloat16)}
    for key, name in zip(kw, NAMES, strict=True):
        w = jax.random.normal(key, SHAPES[name], jnp.float32) * SHAPES[name][1] ** -0.5
        drawn[name] = (w * {"w_gate": 1.0, "w_up": bump(kh, FF, 4.0), "w_down": layers}[name]).astype(jnp.bfloat16)
    for key, name in zip(km, NAMES, strict=True):
        drawn[f"m_{name}"] = 0.1 * jax.random.normal(key, SHAPES[name], jnp.float32)
    for key, name in zip(kv, NAMES, strict=True):
        drawn[f"v_{name}"] = jax.random.uniform(key, SHAPES[name], jnp.float32, 0.005, 0.015)
    return drawn


def matmul(a, w):
    return jnp.dot(a, w, preferred_element_type=jnp.float32).astype(jnp.bfloat16)


def normed(h):
    wide = h.astype(jnp.float32)
    scale = lax.rsqrt(jnp.mean(wide**2, -1, keepdims=True) + 1e-6)
    return (wide * scale).astype(jnp.bfloat16)


def layer(h, w):
    a = normed(h)
    gate = jnp.dot(a, w["w_gate"], preferred_element_type=jnp.float32)
    up = jnp.dot(a, w["w_up"], preferred_element_type=jnp.float32)
    return h + matmul((jax.nn.silu(gate) * up).astype(jnp.bfloat16), w["w_down"])


def adamw(w, m, v, g):
    m = 0.9 * m + 0.1 * g
    v = 0.95 * v + 0.05 * g * g
    step = m * lax.rsqrt(v + 1e-8) + 0.1 * w
    return (w - 0.02 * step).astype(jnp.bfloat16), m, v


def stack(weights, h):
    return lax.scan(lambda h, w: (layer(h, w), None), h, weights)[0]


def reference(x, dy, w_gate, w_up, w_down, m_w_gate, m_w_up, m_w_down, v_w_gate, v_w_up, v_w_down):
    weights = dict(zip(NAMES, (w_gate, w_up, w_down), strict=True))

    def take(so_far, sequence):
        h, by_y = sequence
        _, back = jax.vjp(lambda w: stack(w, h), weights)
        return jax.tree.map(lambda total, term: total + term.astype(jnp.float32), so_far, back(by_y)[0]), None

    none_yet = {name: jnp.zeros(w.shape, jnp.float32) for name, w in weights.items()}
    by_weights, _ = lax.scan(take, none_yet, (x, dy))
    gradients = [by_weights[name].astype(jnp.bfloat16).astype(jnp.float32) for name in NAMES]
    new = [
        adamw(w.astype(jnp.float32), m, v, g)
        for w, m, v, g in zip((w_gate, w_up, w_down), (m_w_gate, m_w_up, m_w_down), (v_w_gate, v_w_up, v_w_down), gradients, strict=True)
    ]
    return tuple(one[which] for which in range(3) for one in new)
```

```python
import functools
import math

import jax
import jax.numpy as jnp
from jax import lax
from jax.experimental import pallas as pl
from jax.experimental.pallas import tpu as pltpu
from jax.sharding import PartitionSpec as P

F32, BF16 = jnp.float32, jnp.bfloat16
MESH = pl.DeviceIdType.MESH
ANY = pl.BlockSpec(memory_space=pl.ANY)
PARTS = 3
TILE = 512


def mm(a, w):
    return lax.dot_general(a, w, (((1,), (0,)), ((), ())), preferred_element_type=F32)


def mm_t(a, w):
    return lax.dot_general(a, w, (((1,), (1,)), ((), ())), preferred_element_type=F32)


def t_mm(a, d):
    return lax.dot_general(a, d, (((0,), (0,)), ((), ())), preferred_element_type=F32)


def normed(h):
    wide = h.astype(F32)
    scale = lax.rsqrt(jnp.mean(wide**2, -1, keepdims=True) + 1e-6)
    return (wide * scale).astype(BF16)


def by_normed(h, by_a):
    wide, by = h.astype(F32), by_a.astype(F32)
    scale = lax.rsqrt(jnp.mean(wide**2, -1, keepdims=True) + 1e-6)
    return (scale * by - wide * (scale**3 * jnp.mean(wide * by, -1, keepdims=True))).astype(BF16)


def adamw(w, m, v, g):
    m = 0.9 * m + 0.1 * g
    v = 0.95 * v + 0.05 * g * g
    step = m * lax.rsqrt(v + 1e-8) + 0.1 * w
    return (w - 0.02 * step).astype(BF16), m, v


def other(me, bit):
    return me + bit - 2 * bit * ((me // bit) % 2)


def remote(src, dst, sems, n, bit):
    return pltpu.make_async_remote_copy(
        src_ref=src,
        dst_ref=dst,
        send_sem=sems[0].at[n],
        recv_sem=sems[1].at[n],
        device_id={"dp": other(lax.axis_index("dp"), bit)},
        device_id_type=MESH,
    )


class Gather:
    bits = (2, 4)

    def __init__(self, block):
        _, r, n = block.shape
        self.ins = [block]
        self.outs = [jax.ShapeDtypeStruct((8, r, n), block.dtype)]
        self.scratch = [pltpu.VMEM((2, r, n), block.dtype), pltpu.SemaphoreType.DMA((2,)), pltpu.SemaphoreType.DMA((6,)), pltpu.SemaphoreType.DMA((6,))]

    def bind(self, ins, outs, scratch):
        (block,), (full,), (held, local, *sems) = ins, outs, scratch
        chip = lax.axis_index("dp") // 2
        at = lambda bit, half: full.at[other(chip, bit) * 2 + half] if bit else full.at[chip * 2 + half]
        self.copies = [
            remote(block.at[1], at(0, 1), sems, 0, 2),
            remote(block.at[0], at(0, 0), sems, 1, 4),
            remote(block.at[0], at(0, 0), sems, 2, 2),
            remote(block.at[1], at(0, 1), sems, 3, 4),
            remote(at(2, 0), at(2, 0), sems, 4, 2),
            remote(at(1, 1), at(1, 1), sems, 5, 4),
        ]
        self.own = [pltpu.make_async_copy(block, held, local.at[0]), pltpu.make_async_copy(held, full.at[pl.ds(chip * 2, 2)], local.at[1])]

    def begin(self):
        for copy in self.copies[:4]:
            copy.start()
        self.own[0].start()

    def middle(self):
        self.own[0].wait()
        self.own[1].start()
        self.copies[1].wait_recv()
        self.copies[4].start()
        self.copies[0].wait_recv()
        self.copies[5].start()

    def late(self):
        pass

    def end(self):
        for n in (2, 3, 4, 5):
            self.copies[n].wait_recv()
        for copy in self.copies:
            copy.wait_send()
        self.own[1].wait()


class Scatter:
    bits = (2, 4)

    def __init__(self, blocks):
        _, r, n = blocks.shape
        self.ins = [blocks]
        self.outs = [jax.ShapeDtypeStruct((2, r, n), BF16)] * 2
        self.scratch = [pltpu.VMEM((2, r, n), BF16)] * 3 + [pltpu.SemaphoreType.DMA((2,)), pltpu.SemaphoreType.DMA((6,)), pltpu.SemaphoreType.DMA((6,))]

    def bind(self, ins, outs, scratch):
        (blocks,), (by_y, by_x), (came, mine, total, local, *sems) = ins, outs, scratch
        chip = lax.axis_index("dp") // 2
        at = lambda bit, half: blocks.at[other(chip, bit) * 2 + half]
        diagonal = lambda half: blocks.at[(3 - chip) * 2 + half]
        self.came, self.mine, self.total = came, mine, total
        self.copies = [
            remote(diagonal(0), came.at[0], sems, 0, 4),
            remote(diagonal(1), came.at[1], sems, 1, 2),
            remote(at(2, 0), by_x.at[0], sems, 2, 4),
            remote(at(1, 1), by_y.at[1], sems, 3, 2),
            remote(total.at[0], by_y.at[0], sems, 4, 2),
            remote(total.at[1], by_x.at[1], sems, 5, 4),
        ]
        self.own = [pltpu.make_async_copy(at(1, 0), mine.at[0], local.at[0]), pltpu.make_async_copy(at(2, 1), mine.at[1], local.at[1])]

    def begin(self):
        for copy in self.copies[:4]:
            copy.start()
        for copy in self.own:
            copy.start()

    def middle(self):
        for half in range(2):
            self.copies[half].wait_recv()
            self.own[half].wait()
            self.total[half] = (self.came[half].astype(F32) + self.mine[half].astype(F32)).astype(BF16)

    def late(self):
        self.copies[4].start()
        self.copies[5].start()

    def end(self):
        for n in (2, 3, 4, 5):
            self.copies[n].wait_recv()
        for copy in self.copies:
            copy.wait_send()


def run(name, cid, compute, grid, ins, in_specs, outs, out_specs, scratch=(), comms=(), bits=(), when=(0.4, 0.5), flops=0):
    steps = math.prod(grid)
    bits = sorted(set(bits).union(*(comm.bits for comm in comms)))
    middle, late = (min(steps - 1, int(steps * w)) for w in when)
    counts = [len(ins)] + [len(c.ins) for c in comms] + [len(outs)] + [len(c.outs) for c in comms] + [len(scratch)] + [len(c.scratch) for c in comms]

    def kernel(*refs):
        refs, groups = list(refs), []
        for count in counts:
            groups.append(refs[:count])
            refs = refs[count:]
        step = 0
        for axis, size in enumerate(grid):
            step = step * size + pl.program_id(axis)
        k = len(comms) + 1
        own = groups[0], groups[k], groups[2 * k]
        for n, comm in enumerate(comms):
            comm.bind(groups[1 + n], groups[k + 1 + n], groups[2 * k + 1 + n])

        @pl.when(step == 0)
        def _():
            if bits:
                barrier = pltpu.get_barrier_semaphore()
                for bit in bits:
                    pl.semaphore_signal(barrier, inc=1, device_id={"dp": other(lax.axis_index("dp"), bit)}, device_id_type=MESH)
                pl.semaphore_wait(barrier, len(bits))
            for comm in comms:
                comm.begin()

        compute(*own)
        for at, what in ((middle, "middle"), (late, "late"), (steps - 1, "end")):
            if comms:

                @pl.when(step == at)
                def _():
                    for comm in comms:
                        getattr(comm, what)()

    params = dict(collective_id=cid, has_side_effects=True) if bits else {}
    results = pl.pallas_call(
        kernel,
        name=name,
        grid=grid,
        in_specs=list(in_specs) + [ANY for c in comms for _ in c.ins],
        out_specs=list(out_specs) + [ANY for c in comms for _ in c.outs],
        out_shape=list(outs) + [o for c in comms for o in c.outs],
        scratch_shapes=list(scratch) + [s for c in comms for s in c.scratch],
        compiler_params=pltpu.CompilerParams(dimension_semantics=("arbitrary",) * len(grid), vmem_limit_bytes=62 * 2**20, **params),
        cost_estimate=pl.CostEstimate(flops=int(flops), bytes_accessed=0, transcendentals=0),
    )(*ins, *[a for c in comms for a in c.ins])
    return results[: len(outs)], results[len(outs) :]


def solution(mesh):
    size = mesh.shape["dp"]
    chips = size // 2
    pairs = [(i, i ^ 1) for i in range(size)]

    def sibling(a):
        return lax.ppermute(a, "dp", pairs)

    def step(x, dy, *arrays):
        weights, m, v = (arrays[i : i + 3] for i in (0, 3, 6))
        first = lax.axis_index("dp") % 2 == 0
        chip = lax.axis_index("dp") // 2
        layers, rows, ff = weights[0].shape
        d = rows * size
        half = ff // 2
        part = half // PARTS
        share = part // chips
        tokens = x.shape[1]
        every = 2 * tokens
        unit = 2 * every * d * half

        def split(w):
            even, odd = jnp.moveaxis(w.reshape(rows, chips, 2, PARTS, share), (2, 3), (0, 2)).reshape(2, rows, half)
            return jnp.where(first, even, odd), jnp.where(first, odd, even)

        def join(mine, theirs):
            both = jnp.stack([jnp.where(first, mine, theirs), jnp.where(first, theirs, mine)])
            return jnp.moveaxis(both.reshape(2, rows, PARTS, chips, share), (0, 2), (2, 3)).reshape(rows, ff)

        def in_order(mine, theirs):
            return jnp.stack([jnp.where(first, mine, theirs), jnp.where(first, theirs, mine)])

        blocks = {}
        for n in range(layers):
            for i in range(2):
                mine, give = split(weights[i][n])
                blocks[i, n] = in_order(mine, sibling(give))
            blocks[2, n] = weights[2][n].reshape(2, -1, d)

        def both(a):
            return jnp.concatenate([a, sibling(a)])

        cid = iter(range(100))
        wide = every // 4
        col, row = lambda n: pl.BlockSpec((wide, n), lambda j, i: (i, 0)), pl.BlockSpec((wide, part), lambda j, i: (i, j))
        weight = pl.BlockSpec((d, part), lambda j, i: (0, j))
        f32_rows, bf16_rows = jax.ShapeDtypeStruct((every, half), F32), jax.ShapeDtypeStruct((every, half), BF16)

        def gate_of(a, w, fetch):
            def compute(ins, outs, _):
                outs[0][...] = mm(ins[0][...], ins[1][...])

            (gate,), (got,) = run("gate", next(cid), compute, (PARTS, 4), [a, w], [col(d), weight], [f32_rows], [row], comms=[Gather(fetch)], flops=unit)
            return gate, got

        def up_of(a, w, gate, fetch):
            def compute(ins, outs, _):
                up, gate = mm(ins[0][...], ins[1][...]), ins[2][...]
                outs[0][...] = up
                outs[1][...] = (jax.nn.silu(gate) * up).astype(BF16)

            (up, hidden), (got,) = run(
                "up", next(cid), compute, (PARTS, 4), [a, w, gate], [col(d), weight, row], [f32_rows, bf16_rows], [row, row], comms=[Gather(fetch)], flops=unit
            )
            return up, hidden, got

        def over_cores(name, terms, lhs, lhs_specs, rhs, given, finish, keep, comms):
            tiles = tokens // TILE
            here = pl.BlockSpec((TILE, d), lambda t: (jnp.maximum(t - tiles, 0), 0))

            def compute(ins, outs, scratch):
                sent, came, state, ssem, rsem, ssem2, rsem2, local = scratch
                t = pl.program_id(0)
                total = terms(ins[: len(lhs)], ins[len(lhs) : len(lhs) + len(rhs)])
                away = lambda n: remote(sent.at[n], came.at[n], (ssem, rsem), n, 1)
                shared = outs[-1]
                rows_of = lambda n: pl.ds(n * TILE, TILE)
                tell = lambda n: remote(state.at[n], shared.at[1, rows_of(n)], (ssem2, rsem2), n, 1)
                save = lambda n: pltpu.make_async_copy(state.at[n], shared.at[0, rows_of(n)], local.at[n])

                for n in range(tiles):

                    @pl.when(t == n)
                    def _():
                        sent[n] = total

                    @pl.when(t == n + 1)
                    def _():
                        away(n).start()

                    @pl.when(t == n + tiles)
                    def _():
                        away(n).wait_recv()
                        results = finish(total + came[n], *[g[...] for g in ins[len(lhs) + len(rhs) :]])
                        for out, result in zip(outs[:-1], results[:-1], strict=True):
                            out[...] = result
                        state[n] = results[-1]
                        if n:
                            tell(n - 1).start()
                            save(n - 1).start()

                @pl.when(t == 2 * tiles - 1)
                def _():
                    tell(tiles - 1).start()
                    save(tiles - 1).start()
                    for n in range(tiles):
                        away(n).wait_send()
                        tell(n).wait()
                        save(n).wait()

            scratch = [pltpu.VMEM((tiles, TILE, d), F32)] * 2 + [pltpu.VMEM((tiles, TILE, d), BF16)] + [pltpu.SemaphoreType.DMA((tiles,))] * 5
            whole = lambda a: pl.BlockSpec(a.shape, lambda t: (0,) * a.ndim, pipeline_mode=pl.Buffered(1))
            results, got = run(
                name,
                next(cid),
                compute,
                (2 * tiles,),
                [*lhs, *rhs, *given],
                list(lhs_specs) + [whole(a) for a in rhs] + [here] * len(given),
                [jax.ShapeDtypeStruct((tokens, d), BF16)] * keep + [jax.ShapeDtypeStruct((2, tokens, d), BF16)],
                [here] * keep + [ANY],
                scratch,
                comms=comms,
                bits=(1,),
                flops=unit * len(lhs),
            )
            return [*results[:-1], results[-1].reshape(every, d)], got

        swapped = lambda n: pl.BlockSpec((TILE, n), lambda t: ((t + tokens // TILE) % (every // TILE), 0))

        def down_of(hidden, w, h, fetch):
            def terms(lhs, rhs):
                return sum(mm(lhs[0][:, p * part : (p + 1) * part], rhs[0][:, p].reshape(part, d)) for p in range(PARTS))

            def finish(total, h):
                h = h + total.astype(BF16)
                return h, normed(h)

            (h, a), (got,) = over_cores("down", terms, [hidden], [swapped(half)], [w.reshape(chips, PARTS, share, d)], [h], finish, 1, [Gather(fetch)])
            return h, a, got

        def by_hidden(p, by_h, w, gate, up, a, keep, comms=()):
            n_steps = every // TILE

            def compute(ins, outs, scratch):
                by_h, w, gate, up, a = (r[...] for r in ins)
                by = mm_t(by_h, w.reshape(part, d)).astype(BF16).astype(F32)
                sig = 1 / (1 + jnp.exp(-gate))
                act = gate * sig
                by_up = (by * act).astype(BF16)
                by_gate = (by * up * (sig * (1 + gate * (1 - sig)))).astype(BF16)
                if keep:
                    outs[3][...], outs[4][...] = by_gate, by_up
                t = pl.program_id(0)
                hidden = (act * up).astype(BF16)
                for acc, lhs, rhs in zip(scratch, (a, a, hidden), (by_gate, by_up, by_h), strict=True):

                    @pl.when(t == 0)
                    def _():
                        acc[...] = t_mm(lhs, rhs)

                    @pl.when(t > 0)
                    def _():
                        acc[...] += t_mm(lhs, rhs)

                @pl.when(t == n_steps - 1)
                def _():
                    for acc, out in zip(scratch, outs[:3], strict=True):
                        out[...] = acc[...].astype(BF16)

            tile = lambda n: pl.BlockSpec((TILE, n), lambda t: (t, 0))
            piece = pl.BlockSpec((TILE, part), lambda t: (t, p))
            whole = lambda *s: pl.BlockSpec(s, lambda t: (0,) * len(s), pipeline_mode=pl.Buffered(1))
            outs = [jax.ShapeDtypeStruct((d, part), BF16)] * 2 + [jax.ShapeDtypeStruct((part, d), BF16)]
            out_specs = [whole(d, part)] * 2 + [whole(part, d)]
            if keep:
                outs += [jax.ShapeDtypeStruct((every, part), BF16)] * 2
                out_specs += [tile(part)] * 2
            return run(
                "by_hidden",
                next(cid),
                compute,
                (n_steps,),
                [by_h, w.reshape(chips, PARTS, share, d), gate, up, a],
                [tile(d), pl.BlockSpec((chips, 1, share, d), lambda t: (0, p, 0, 0), pipeline_mode=pl.Buffered(1)), piece, piece, tile(d)],
                outs,
                out_specs,
                [pltpu.VMEM((d, part), F32)] * 2 + [pltpu.VMEM((part, d), F32)],
                comms=comms,
                flops=4 * unit // PARTS,
            )

        def by_input(by_gates, by_ups, wg, wu, h, by_h, comms=()):
            def terms(lhs, rhs):
                return sum(
                    mm_t(lhs[side * PARTS + p][...], rhs[side][:, p * part : (p + 1) * part]) for side in range(2) for p in range(PARTS)
                )

            def finish(total, h, by_h):
                return (by_h + by_normed(h, total.astype(BF16)),)

            lhs = [*by_gates, *by_ups]
            (by_hs,), got = over_cores("by_input", terms, lhs, [swapped(part)] * len(lhs), [wg, wu], [h, by_h], finish, 0, comms)
            return by_hs, got

        def just(comm):
            def compute(*_):
                pass

            return run("gather", next(cid), compute, (1,), [], [], [], [], comms=[comm])[1]

        flat = lambda w: w.reshape(-1, w.shape[-1])
        h0 = x[0]
        a0 = normed(both(h0))
        dys = both(dy[0])
        (wg0,) = just(Gather(blocks[0, 0]))
        gate0, wu0 = gate_of(a0, flat(wg0), blocks[1, 0])
        up0, hidden0, wd0 = up_of(a0, flat(wu0), gate0, blocks[2, 0])
        h1, a1, wg1 = down_of(hidden0, wd0, h0, blocks[0, 1])
        gate1, wu1 = gate_of(a1, flat(wg1), blocks[1, 1])
        up1, hidden1, wd1 = up_of(a1, flat(wu1), gate1, blocks[2, 1])

        pending, mine = None, {}

        def scatters():
            if pending is None:
                return []
            return [Scatter(g.reshape(8, -1, g.shape[-1])) for g in pending[1]]

        def settle(got):
            if pending is not None:
                for i, g in enumerate(pending[1]):
                    own = lax.dynamic_index_in_dim(g.reshape(chips, -1, g.shape[-1]), chip, keepdims=False)
                    terms = [own] + [t.reshape(own.shape) for t in got[2 * i : 2 * i + 2]]
                    mine[pending[0] + (i,)] = sum(t.astype(F32) for t in terms).astype(BF16)

        kept = {0: (wd0, gate0, up0, a0), 1: (wd1, gate1, up1, a1)}
        by_hs = dys
        for n in (1, 0):
            by_gates, by_ups = [], []
            for p in range(PARTS):
                results, got = by_hidden(p, by_hs, *kept[n], bool(n), scatters())
                settle(got)
                pending = ((n, p), results[:3])
                by_gates += results[3:4]
                by_ups += results[4:5]
            if n:
                by_hs, got = by_input(by_gates, by_ups, flat(wg1), flat(wu1), h1, dy[0], scatters())
                settle(got)
                pending = None
        got = run("last", next(cid), lambda *_: None, (1,), [], [], [], [], comms=scatters())[1]
        settle(got)

        gradients = []
        for i in range(2):
            each = []
            for n in range(layers):
                got = jnp.concatenate([mine[n, p, i] for p in range(PARTS)], axis=1)
                top, bottom = got[:rows], got[rows:]
                each.append(join(jnp.where(first, top, bottom), sibling(jnp.where(first, bottom, top))))
            gradients.append(jnp.stack(each))
        gradients.append(jnp.stack([jnp.concatenate([mine[n, p, 2] for p in range(PARTS)]) for n in range(layers)]))
        new = [adamw(w.astype(F32), m, v, g.astype(F32)) for w, m, v, g in zip(weights, m, v, gradients, strict=True)]
        return tuple(one[which] for which in range(3) for one in new)

    states, cut = P(("rep", "dp"), None, None), P(None, "dp", None)
    return jax.shard_map(
        step,
        mesh=mesh,
        in_specs=(states, states) + (cut,) * 9,
        out_specs=(P("rep", "dp", None),) * 9,
        check_vma=False,
    )
```

```python
import functools
import math

import jax
import jax.numpy as jnp
from jax import lax
from jax.experimental import pallas as pl
from jax.experimental.pallas import tpu as pltpu
from jax.sharding import PartitionSpec as P

F32, BF16 = jnp.float32, jnp.bfloat16
MESH = pl.DeviceIdType.MESH
ANY = pl.BlockSpec(memory_space=pl.ANY)
PARTS = 3
TILE = 512


def mm(a, w):
    return lax.dot_general(a, w, (((1,), (0,)), ((), ())), preferred_element_type=F32)


def mm_t(a, w):
    return lax.dot_general(a, w, (((1,), (1,)), ((), ())), preferred_element_type=F32)


def t_mm(a, d):
    return lax.dot_general(a, d, (((0,), (0,)), ((), ())), preferred_element_type=F32)


def normed(h):
    wide = h.astype(F32)
    scale = lax.rsqrt(jnp.mean(wide**2, -1, keepdims=True) + 1e-6)
    return (wide * scale).astype(BF16)


def by_normed(h, by_a):
    wide, by = h.astype(F32), by_a.astype(F32)
    scale = lax.rsqrt(jnp.mean(wide**2, -1, keepdims=True) + 1e-6)
    return (scale * by - wide * (scale**3 * jnp.mean(wide * by, -1, keepdims=True))).astype(BF16)


def adamw(w, m, v, g):
    m = 0.9 * m + 0.1 * g
    v = 0.95 * v + 0.05 * g * g
    step = m * lax.rsqrt(v + 1e-8) + 0.1 * w
    return (w - 0.02 * step).astype(BF16), m, v


def other(me, bit):
    return me + bit - 2 * bit * ((me // bit) % 2)


def remote(src, dst, sems, n, bit):
    return pltpu.make_async_remote_copy(
        src_ref=src,
        dst_ref=dst,
        send_sem=sems[0].at[n],
        recv_sem=sems[1].at[n],
        device_id={"dp": other(lax.axis_index("dp"), bit)},
        device_id_type=MESH,
    )


class Gather:
    bits = (2, 4)

    def __init__(self, block, source=None, index=None):
        _, r, n = block.shape[-3:]
        self.source = source
        self.index = index
        self.ins = [] if source else [block]
        self.outs = [jax.ShapeDtypeStruct((8, r, n), block.dtype)]
        self.scratch = [pltpu.VMEM((2, r, n), block.dtype), pltpu.SemaphoreType.DMA((2,)), pltpu.SemaphoreType.DMA((6,)), pltpu.SemaphoreType.DMA((6,))]

    def bind(self, ins, outs, scratch, own):
        (full,), (held, local, *sems) = outs, scratch
        block = self.source(own) if self.source else ins[0] if self.index is None else ins[0].at[self.index]
        chip = lax.axis_index("dp") // 2
        at = lambda bit, half: full.at[other(chip, bit) * 2 + half] if bit else full.at[chip * 2 + half]
        self.copies = [
            remote(block.at[1], at(0, 1), sems, 0, 2),
            remote(block.at[0], at(0, 0), sems, 1, 4),
            remote(block.at[0], at(0, 0), sems, 2, 2),
            remote(block.at[1], at(0, 1), sems, 3, 4),
            remote(at(2, 0), at(2, 0), sems, 4, 2),
            remote(at(1, 1), at(1, 1), sems, 5, 4),
        ]
        self.own = [pltpu.make_async_copy(block, held, local.at[0]), pltpu.make_async_copy(held, full.at[pl.ds(chip * 2, 2)], local.at[1])]

    def begin(self):
        for copy in (*self.copies[:2], self.own[0]):
            copy.start()

    def more(self):
        for copy in self.copies[2:4]:
            copy.start()

    def middle(self):
        self.own[0].wait()
        self.own[1].start()
        self.copies[1].wait_recv()
        self.copies[4].start()
        self.copies[0].wait_recv()
        self.copies[5].start()

    def late(self):
        pass

    def end(self):
        for n in (2, 3, 4, 5):
            self.copies[n].wait_recv()

    def finish(self):
        pass

    def close(self):
        for copy in self.copies:
            copy.wait_send()
        self.own[1].wait()


class Scatter:
    bits = (1, 2, 4)

    def __init__(self, blocks, rows):
        _, r, n = blocks.shape
        self.ins, self.rows = [blocks], rows
        self.outs = [jax.ShapeDtypeStruct((r, n), BF16)] * 2 if rows else [jax.ShapeDtypeStruct((2, r, n), BF16)]
        self.scratch = [pltpu.VMEM((2, r, n), BF16)] * 6 + [pltpu.SemaphoreType.DMA((4,))] + [pltpu.SemaphoreType.DMA((7,))] * 2

    def bind(self, ins, outs, scratch, own):
        (blocks,), (came, mine, total, by_y, by_x, held, local, *sems) = ins, scratch
        core, chip = lax.axis_index("dp") % 2, lax.axis_index("dp") // 2
        at = lambda bit, half: blocks.at[other(chip, bit) * 2 + half]
        diagonal = lambda half: blocks.at[(3 - chip) * 2 + half]
        self.came, self.mine, self.total, self.by_y, self.by_x, self.held = came, mine, total, by_y, by_x, held
        self.copies = [
            remote(diagonal(0), came.at[0], sems, 0, 4),
            remote(diagonal(1), came.at[1], sems, 1, 2),
            remote(at(2, 0), by_x.at[0], sems, 2, 4),
            remote(at(1, 1), by_y.at[1], sems, 3, 2),
            remote(total.at[0], by_y.at[0], sems, 4, 2),
            remote(total.at[1], by_x.at[1], sems, 5, 4),
        ]
        self.own = [pltpu.make_async_copy(at(1, 0), mine.at[0], local.at[0]), pltpu.make_async_copy(at(2, 1), mine.at[1], local.at[1])]
        self.own += [pltpu.make_async_copy(blocks.at[pl.ds(chip * 2, 2)], held, local.at[2])]
        if self.rows:
            self.out = pltpu.make_async_copy(held.at[core], outs[0], local.at[3])
            self.tell = remote(held.at[1 - core], outs[1], sems, 6, 1)
        else:
            self.out = pltpu.make_async_copy(held, outs[0], local.at[3])

    def begin(self):
        for copy in (*self.copies[:2], *self.own):
            copy.start()

    def more(self):
        for copy in self.copies[2:4]:
            copy.start()

    def middle(self):
        for half in range(2):
            self.copies[half].wait_recv()
            self.own[half].wait()
            self.total[half] = (self.came[half].astype(F32) + self.mine[half].astype(F32)).astype(BF16)

    def late(self):
        self.copies[4].start()
        self.copies[5].start()

    def end(self):
        for n in (2, 3, 4, 5):
            self.copies[n].wait_recv()
        self.own[2].wait()
        self.held[...] = (self.held[...].astype(F32) + self.by_y[...].astype(F32) + self.by_x[...].astype(F32)).astype(BF16)

    def finish(self):
        self.out.start()
        if self.rows:
            self.tell.start()

    def close(self):
        for copy in self.copies:
            copy.wait_send()
        self.out.wait()
        if self.rows:
            self.tell.wait()


def run(name, cid, compute, grid, ins, in_specs, outs, out_specs, scratch=(), comms=(), bits=(), when=(0.4, 0.5), flops=0, start=0):
    steps = math.prod(grid)
    bits = sorted(set(bits).union(*(comm.bits for comm in comms)))
    middle, late = (min(steps - 1, int(steps * w)) for w in when)
    counts = [len(ins)] + [len(c.ins) for c in comms] + [len(outs)] + [len(c.outs) for c in comms] + [len(scratch)] + [len(c.scratch) for c in comms]

    def kernel(*refs):
        refs, groups = list(refs), []
        for count in counts:
            groups.append(refs[:count])
            refs = refs[count:]
        step = 0
        for axis, size in enumerate(grid):
            step = step * size + pl.program_id(axis)
        k = len(comms) + 1
        own = groups[0], groups[k], groups[2 * k]
        for n, comm in enumerate(comms):
            comm.bind(groups[1 + n], groups[k + 1 + n], groups[2 * k + 1 + n], own)

        def do(*names):
            for what in names:
                for comm in comms:
                    getattr(comm, what)()

        @pl.when(step == 0)
        def _():
            if bits:
                barrier = pltpu.get_barrier_semaphore()
                for bit in bits:
                    pl.semaphore_signal(barrier, inc=1, device_id={"dp": other(lax.axis_index("dp"), bit)}, device_id_type=MESH)
                pl.semaphore_wait(barrier, len(bits))
            if not start:
                do("begin", "more")

        compute(*own)
        for at, what in ((start, ("begin", "more")), (middle, ("middle",)), (late, ("late",)), (steps - 1, ("end", "finish", "close"))):
            if comms and (start or at or what[0] != "begin"):

                @pl.when(step == at)
                def _():
                    do(*what)

    params = dict(collective_id=cid, has_side_effects=True) if bits else {}
    results = pl.pallas_call(
        kernel,
        name=name,
        grid=grid,
        in_specs=list(in_specs) + [ANY for c in comms for _ in c.ins],
        out_specs=list(out_specs) + [ANY for c in comms for _ in c.outs],
        out_shape=list(outs) + [o for c in comms for o in c.outs],
        scratch_shapes=list(scratch) + [s for c in comms for s in c.scratch],
        compiler_params=pltpu.CompilerParams(dimension_semantics=("arbitrary",) * len(grid), vmem_limit_bytes=62 * 2**20, **params),
        cost_estimate=pl.CostEstimate(flops=int(flops), bytes_accessed=0, transcendentals=0),
    )(*ins, *[a for c in comms for a in c.ins])
    results, got = results[: len(outs)], list(results[len(outs) :])
    return results, [[got.pop(0) for _ in comm.outs] for comm in comms]


def solution(mesh):
    size = mesh.shape["dp"]
    chips = size // 2

    def step(x, dy, *arrays):
        weights, m, v = (arrays[i : i + 3] for i in (0, 3, 6))
        layers, rows, ff = weights[0].shape
        d = rows * size
        half = ff // 2
        part = half // PARTS
        share = part // chips
        tokens = x.shape[1]
        every = 2 * tokens
        unit = 2 * every * d * half

        segments = lambda core: [(c * 2 * PARTS * share + core * PARTS * share + p * share, p * part + c * share) for p in range(PARTS) for c in range(chips)]

        cid = iter(range(100))
        wide = every // 4
        col, row = lambda n: pl.BlockSpec((wide, n), lambda j, i: (i, 0)), pl.BlockSpec((wide, part), lambda j, i: (i, j))
        weight = pl.BlockSpec((d, part), lambda j, i: (0, j))
        f32_rows, bf16_rows = jax.ShapeDtypeStruct((every, half), F32), jax.ShapeDtypeStruct((every, half), BF16)

        def gate_of(a, w, fetch):
            def compute(ins, outs, _):
                outs[0][...] = mm(ins[0][...], ins[1][...])

            (gate,), ((got,),) = run("gate", next(cid), compute, (PARTS, 4), [a, w], [col(d), weight], [f32_rows], [row], comms=[fetch], flops=unit)
            return gate, got

        def up_of(a, w, gate, fetch):
            def compute(ins, outs, _):
                up, gate = mm(ins[0][...], ins[1][...]), ins[2][...]
                outs[0][...] = up
                outs[1][...] = (jax.nn.silu(gate) * up).astype(BF16)

            tile = lambda n: pl.BlockSpec((TILE, n), lambda t: (t, 0))
            whole = pl.BlockSpec((d, half), lambda t: (0, 0), pipeline_mode=pl.Buffered(1))
            (up, hidden), ((got,),) = run(
                "up",
                next(cid),
                compute,
                (every // TILE,),
                [a, w, gate],
                [tile(d), whole, tile(half)],
                [f32_rows, bf16_rows],
                [tile(half)] * 2,
                comms=[fetch],
                flops=unit,
            )
            return up, hidden, got

        def over_cores(name, terms, lhs, lhs_specs, rhs, given, finish, keep, comms):
            tiles = tokens // TILE
            here = pl.BlockSpec((TILE, d), lambda t: (jnp.maximum(t - tiles, 0), 0))

            def compute(ins, outs, scratch):
                sent, came, state, ssem, rsem, ssem2, rsem2, local = scratch
                t = pl.program_id(0)
                product = lambda: terms(ins[: len(lhs)], ins[len(lhs) : len(lhs) + len(rhs)])
                away = lambda n: remote(sent.at[n], came.at[n], (ssem, rsem), n, 1)
                shared = outs[-1]
                rows_of = lambda n: pl.ds(pl.multiple_of(n * TILE, TILE), TILE)
                tell = lambda n: remote(state.at[n], shared.at[1, rows_of(n)], (ssem2, rsem2), n, 1)
                save = lambda n: pltpu.make_async_copy(state.at[n], shared.at[0, rows_of(n)], local.at[n])
                n = t - tiles

                @pl.when((t > 0) & (t <= tiles))
                def _():
                    away(t - 1).start()

                @pl.when(n > 0)
                def _():
                    tell(n - 1).start()
                    save(n - 1).start()

                @pl.when(t < tiles)
                def _():
                    sent[t] = product()

                @pl.when(n >= 0)
                def _():
                    away(n).wait_recv()
                    results = finish(product() + came[n], *[g[...] for g in ins[len(lhs) + len(rhs) :]])
                    for out, result in zip(outs[:-1], results[:-1], strict=True):
                        out[...] = result
                    state[n] = results[-1]

                @pl.when(n == tiles - 1)
                def _():
                    tell(tiles - 1).start()
                    save(tiles - 1).start()
                    for n in range(tiles):
                        away(n).wait_send()
                        tell(n).wait()
                        save(n).wait()

            scratch = [pltpu.VMEM((tiles, TILE, d), F32)] * 2 + [pltpu.VMEM((tiles, TILE, d), BF16)] + [pltpu.SemaphoreType.DMA((tiles,))] * 5
            whole = lambda a: pl.BlockSpec(a.shape, lambda t: (0,) * a.ndim, pipeline_mode=pl.Buffered(1))
            results, got = run(
                name,
                next(cid),
                compute,
                (2 * tiles,),
                [*lhs, *rhs, *given],
                list(lhs_specs) + [whole(a) for a in rhs] + [here] * len(given),
                [jax.ShapeDtypeStruct((tokens, d), BF16)] * keep + [jax.ShapeDtypeStruct((2, tokens, d), BF16)],
                [here] * keep + [ANY],
                scratch,
                comms=comms,
                bits=(1,),
                flops=unit * len(lhs),
            )
            return [*results[:-1], results[-1].reshape(every, d)], got

        swapped = lambda n: pl.BlockSpec((TILE, n), lambda t: ((t + tokens // TILE) % (every // TILE), 0))

        def down_of(hidden, w, h, fetches):
            def terms(lhs, rhs):
                return sum(mm(lhs[0][:, p * part : (p + 1) * part], rhs[0][:, p].reshape(part, d)) for p in range(PARTS))

            def finish(total, h):
                h = h + total.astype(BF16)
                return h, normed(h)

            (h, a), got = over_cores("down", terms, [hidden], [swapped(half)], [w.reshape(chips, PARTS, share, d)], [h], finish, 1, fetches)
            return h, a, got

        def by_hidden(by_h, a, given, given_specs, start, keep, comms=()):
            n_steps = every // TILE

            def compute(ins, outs, scratch):
                t = pl.program_id(0)

                @pl.when(t == 0)
                def _():
                    for acc in scratch:
                        acc[...] = jnp.zeros_like(acc)

                by_h, a = ins[0][...], ins[1][...]
                gate, up, by = start(by_h, a, *[r[...] for r in ins[2:]])
                sig = 1 / (1 + jnp.exp(-gate))
                act = gate * sig
                by_up = (by * act).astype(BF16)
                by_gate = (by * up * (sig * (1 + gate * (1 - sig)))).astype(BF16)
                hidden = (act * up).astype(BF16)
                if keep:
                    outs[3][...], outs[4][...] = by_gate, by_up
                for acc, lhs, rhs in zip(scratch, (a, a, hidden), (by_gate, by_up, by_h), strict=True):
                    acc[...] += t_mm(lhs, rhs)

                @pl.when(t == n_steps - 1)
                def _():
                    for acc, out in zip(scratch, outs[:3], strict=True):
                        out[...] = acc[...].astype(BF16)

            tile = lambda n: pl.BlockSpec((TILE, n), lambda t: (t, 0))
            outs = [jax.ShapeDtypeStruct((d, part), BF16)] * 2 + [jax.ShapeDtypeStruct((part, d), BF16)]
            out_specs = [whole(d, part)] * 2 + [whole(part, d)]
            if keep:
                outs += [jax.ShapeDtypeStruct((every, part), BF16)] * 2
                out_specs += [tile(part)] * 2
            return run(
                "by_hidden",
                next(cid),
                compute,
                (n_steps,),
                [by_h, a, *given],
                [tile(d), tile(d), *given_specs],
                outs,
                out_specs,
                [pltpu.VMEM((d, part), F32)] * 2 + [pltpu.VMEM((part, d), F32)],
                comms=comms,
                flops=(6 if keep else 4) * unit // PARTS,
            )

        whole = lambda *s: pl.BlockSpec(s, lambda t: (0,) * len(s), pipeline_mode=pl.Buffered(1))

        def by_last(by_h, a, wg, wu, wd, comms):
            def start(by_h, a, wg, wu, wd):
                return mm(a, wg), mm(a, wu), mm_t(by_h, wd).astype(BF16).astype(F32)

            return by_hidden(by_h, a, [wg, wu, wd], [whole(d, part)] * 2 + [whole(part, d)], start, True, comms)

        def by_first(p, by_h, a, gate, up, wd, comms):
            def start(by_h, a, gate, up, wd):
                return gate, up, mm_t(by_h, wd.reshape(part, d)).astype(BF16).astype(F32)

            piece = pl.BlockSpec((TILE, part), lambda t: (t, p))
            rows_of = pl.BlockSpec((chips, 1, share, d), lambda t: (0, p, 0, 0), pipeline_mode=pl.Buffered(1))
            return by_hidden(by_h, a, [gate, up, wd.reshape(chips, PARTS, share, d)], [piece, piece, rows_of], start, False, comms)

        def by_input(by_gates, by_ups, wg, wu, h, by_h, comms=()):
            def terms(lhs, rhs):
                return sum(
                    mm_t(each[...], w[...]) for each, w in zip(lhs, rhs, strict=True)
                )

            def finish(total, h, by_h):
                return (by_h + by_normed(h, total.astype(BF16)),)

            lhs = [*by_gates, *by_ups]
            (by_hs,), got = over_cores("by_input", terms, lhs, [swapped(part)] * len(lhs), [*wg, *wu], [h, by_h], finish, 0, comms)
            return by_hs, got

        def opened(x, dy, w_gate, w_up):
            tiles = tokens // TILE
            count = 2 * layers

            def compute(ins, outs, scratch):
                mine, give, normal, by, ssem, rsem, local, ssem2, rsem2, local2 = scratch
                *blocks, a, dys = outs
                s = pl.program_id(0)
                core = lax.axis_index("dp") % 2
                moved = lambda n: (n,) if n < 2 else range(2 + (n - 2) * PARTS, 2 + (n - 1) * PARTS)
                pieces = lambda ref, m: ref.at[m] if m < 2 else ref.at[2 + (m - 2) // PARTS, :, pl.ds((m - 2) % PARTS * part, part)]
                keep = lambda m: pltpu.make_async_copy(pieces(mine, m), blocks[m].at[core], local.at[m])
                pass_on = lambda m: remote(pieces(give, m), blocks[m].at[core], (ssem, rsem), m, 1)
                rows_of = lambda n: pl.ds(n * TILE, TILE)
                shared = lambda n: [
                    each
                    for i, (state, out) in enumerate(((normal, a), (by, dys)))
                    for each in (
                        remote(state.at[n], out.at[1, rows_of(n)], (ssem2.at[i], rsem2.at[i]), n, 1),
                        pltpu.make_async_copy(state.at[n], out.at[0, rows_of(n)], local2.at[i, n]),
                    )
                ]
                for n in range(count):
                    for k in range(2):

                        @pl.when((s == n) & (core == k))
                        def _():
                            w = ins[2 + n % 2]
                            for which, half_of in ((mine, k), (give, 1 - k)):
                                for at, to in segments(half_of):
                                    which[n, :, to : to + share] = w[0, :, at : at + share]

                    @pl.when(s == n + 1)
                    def _():
                        for m in moved(n):
                            keep(m).start()
                            pass_on(m).start()

                @pl.when(s == 2)
                def _():
                    keep(0).wait()
                    pass_on(0).wait_recv()

                for n in range(tiles):

                    @pl.when(s == count + n)
                    def _():
                        normal[n] = normed(ins[0][...])
                        by[n] = ins[1][...]

                    @pl.when(s == count + n + 1)
                    def _():
                        for copy in shared(n):
                            copy.start()

                @pl.when(s == count + tiles)
                def _():
                    pass_on(0).wait_send()
                    for m in range(1, len(blocks)):
                        keep(m).wait()
                        pass_on(m).wait()
                    for n in range(tiles):
                        for copy in shared(n):
                            copy.wait()

            tile = pl.BlockSpec((TILE, d), lambda s: (jnp.clip(s - count, 0, tiles - 1), 0))
            matrix = pl.BlockSpec((1, rows, ff), lambda s: (jnp.minimum(s // 2, layers - 1), 0, 0))
            sem = pltpu.SemaphoreType.DMA
            state = jax.ShapeDtypeStruct((2, tokens, d), BF16)
            made = [jax.ShapeDtypeStruct((2, rows, half), BF16)] * 2 + [jax.ShapeDtypeStruct((2, rows, part), BF16)] * ((count - 2) * PARTS)
            (*blocks, a, dys), ((got,),) = run(
                "open",
                next(cid),
                compute,
                (count + tiles + 1,),
                [x, dy, w_gate, w_up],
                [tile, tile, matrix, matrix],
                [*made, state, state],
                [ANY] * (len(made) + 2),
                [pltpu.VMEM((count, rows, half), BF16)] * 2
                + [pltpu.VMEM((tiles, TILE, d), BF16)] * 2
                + [sem((len(made),))] * 3
                + [sem((2, tiles))] * 3,
                comms=[Gather(jax.ShapeDtypeStruct((2, rows, half), BF16), lambda own: own[1][0])],
                bits=(1,),
                when=(0.999, 0.999),
                start=2,
            )
            return blocks, a.reshape(every, d), dys.reshape(every, d), got

        def updated(pieces):
            tile = rows // PARTS
            keys = [(n, p) for n in range(layers) for p in range(PARTS)]

            def kernel(*refs):
                state, refs = refs[:9], refs[9:]
                given, refs = refs[: 5 * len(keys)], refs[5 * len(keys) :]
                outs, scratch = refs[:9], refs[9:]
                core, layer, t = lax.axis_index("dp") % 2, pl.program_id(0), pl.program_id(1)
                for i, key in enumerate(keys):
                    gate_up, down = given[5 * i : 5 * i + 4], given[5 * i + 4]
                    for k in range(2):

                        @pl.when((core == k) & (layer == key[0]))
                        def _():
                            for which, source in enumerate(gate_up):
                                for at, to in segments(k if which % 2 == 0 else 1 - k):
                                    if to // part == key[1]:
                                        scratch[which // 2][:, at : at + share] = source[:, to % part : to % part + share].astype(F32)

                    @pl.when((layer == key[0]) & (t == key[1]))
                    def _():
                        scratch[2][...] = down[...].reshape(scratch[2].shape).astype(F32)

                for i in range(3):
                    w, m, v = (state[i + 3 * j][0] for j in range(3))
                    outs[i][0], outs[i + 3][0], outs[i + 6][0] = adamw(w.astype(F32), m, v, scratch[i][...])

            block = lambda a: pl.BlockSpec((1, a.shape[1] // PARTS, a.shape[2]), lambda n, t: (n, t, 0))
            given, given_specs = [], []
            for n, p in keys:
                given += pieces[n, p]
                given_specs += [pl.BlockSpec((tile, part), lambda k, t, n=n: (jnp.where(k == n, t, 0), 0))] * 4
                given_specs += [pl.BlockSpec(pieces[n, p][4].shape, lambda k, t: (0, 0, 0), pipeline_mode=pl.Buffered(1))]
            wide = lambda a, dtype: jax.ShapeDtypeStruct(a.shape, dtype)
            return pl.pallas_call(
                kernel,
                name="adamw",
                grid=(layers, PARTS),
                in_specs=[block(a) for a in (*weights, *m, *v)] + given_specs,
                out_specs=[block(a) for a in (*weights, *m, *v)],
                out_shape=[wide(a, BF16) for a in weights] + [wide(a, F32) for a in (*m, *v)],
                scratch_shapes=[pltpu.VMEM((a.shape[1] // PARTS, a.shape[2]), F32) for a in weights],
                compiler_params=pltpu.CompilerParams(dimension_semantics=("arbitrary",) * 2, vmem_limit_bytes=62 * 2**20),
            )(*weights, *m, *v, *given)

        flat = lambda w: w.reshape(-1, w.shape[-1])
        h0 = x[0]
        down_all = Gather(weights[2].reshape(layers, 2, -1, d), index=0)
        down_part = lambda p: Gather(weights[2].reshape(layers, PARTS, 2, -1, d), index=(1, p))
        (_, up_block, *parts), a0, dys, wg0 = opened(h0, dy[0], weights[0], weights[1])
        fetch = [[Gather(parts[p]), Gather(parts[PARTS + p]), down_part(p)] for p in range(PARTS)]
        gate0, wu0 = gate_of(a0, flat(wg0), Gather(up_block))
        up0, hidden0, wd0 = up_of(a0, flat(wu0), gate0, down_all)
        h1, a1, got = down_of(hidden0, wd0, h0, fetch[0])

        def scatters(made):
            return [Scatter(g.reshape(8, -1, g.shape[-1]), i < 2) for i, g in enumerate(made[:3])]

        full = [[flat(w) for (w,) in got]]
        made, sums = [], []
        for p in range(PARTS):
            beside = [[*fetch[1], fetch[2][0]], fetch[2][1:], []][p]
            send = [c for each in made for c in scatters(each)][[0, 0, 2][p] : [0, 2, 6][p]]
            results, got = by_last(dys, a1, *full[p], [*beside, *send])
            made.append(results)
            got_w, got_g = [flat(w) for (w,) in got[: len(beside)]], got[len(beside) :]
            sums += got_g
            if p == 0:
                full += [got_w[:3], got_w[3:]]
            if p == 1:
                full[2] += got_w
        columns = list(zip(*full, strict=True))
        by_hs, got = by_input([r[3] for r in made], [r[4] for r in made], columns[0], columns[1], h1, dy[0], scatters(made[2]))
        sums += got
        mine = {(1, p): sum(sums[3 * p : 3 * p + 3], []) for p in range(PARTS)}
        results = None
        for p in range(PARTS):
            results, got = by_first(p, by_hs, a0, gate0, up0, wd0, scatters(results) if p else [])
            if p:
                mine[0, p - 1] = sum(got, [])
        mine[0, PARTS - 1] = sum(run("last", next(cid), lambda *_: None, (1,), [], [], [], [], comms=scatters(results))[1], [])
        return tuple(updated(mine))

    states, cut = P(("rep", "dp"), None, None), P(None, "dp", None)
    return jax.shard_map(
        step,
        mesh=mesh,
        in_specs=(states, states) + (cut,) * 9,
        out_specs=(P("rep", "dp", None),) * 9,
        check_vma=False,
    )
```

```python
import functools
import math

import jax
import jax.numpy as jnp
from jax import lax
from jax.experimental import pallas as pl
from jax.experimental.pallas import tpu as pltpu
from jax.sharding import PartitionSpec as P

F32, BF16 = jnp.float32, jnp.bfloat16
MESH = pl.DeviceIdType.MESH
ANY = pl.BlockSpec(memory_space=pl.ANY)
PARTS = 3
TILE = 512


def mm(a, w):
    return lax.dot_general(a, w, (((1,), (0,)), ((), ())), preferred_element_type=F32)


def mm_t(a, w):
    return lax.dot_general(a, w, (((1,), (1,)), ((), ())), preferred_element_type=F32)


def t_mm(a, d):
    return lax.dot_general(a, d, (((0,), (0,)), ((), ())), preferred_element_type=F32)


def normed(h):
    wide = h.astype(F32)
    scale = lax.rsqrt(jnp.mean(wide**2, -1, keepdims=True) + 1e-6)
    return (wide * scale).astype(BF16)


def by_normed(h, by_a):
    wide, by = h.astype(F32), by_a.astype(F32)
    scale = lax.rsqrt(jnp.mean(wide**2, -1, keepdims=True) + 1e-6)
    return (scale * by - wide * (scale**3 * jnp.mean(wide * by, -1, keepdims=True))).astype(BF16)


def adamw(w, m, v, g):
    m = 0.9 * m + 0.1 * g
    v = 0.95 * v + 0.05 * g * g
    step = m * lax.rsqrt(v + 1e-8) + 0.1 * w
    return (w - 0.02 * step).astype(BF16), m, v


def other(me, bit):
    return me + bit - 2 * bit * ((me // bit) % 2)


def remote(src, dst, sems, n, bit):
    return pltpu.make_async_remote_copy(
        src_ref=src,
        dst_ref=dst,
        send_sem=sems[0].at[n],
        recv_sem=sems[1].at[n],
        device_id={"dp": other(lax.axis_index("dp"), bit)},
        device_id_type=MESH,
    )


class Gather:
    bits = (2, 4)

    def __init__(self, block, source=None, index=None):
        _, r, n = block.shape[-3:]
        self.source = source
        self.index = index
        self.ins = [] if source else [block]
        self.outs = [jax.ShapeDtypeStruct((8, r, n), block.dtype)]
        self.scratch = [pltpu.VMEM((2, r, n), block.dtype), pltpu.SemaphoreType.DMA((2,)), pltpu.SemaphoreType.DMA((6,)), pltpu.SemaphoreType.DMA((6,))]

    def bind(self, ins, outs, scratch, own):
        (full,), (held, local, *sems) = outs, scratch
        block = self.source(own) if self.source else ins[0] if self.index is None else ins[0].at[self.index]
        chip = lax.axis_index("dp") // 2
        at = lambda bit, half: full.at[other(chip, bit) * 2 + half] if bit else full.at[chip * 2 + half]
        self.copies = [
            remote(block.at[1], at(0, 1), sems, 0, 2),
            remote(block.at[0], at(0, 0), sems, 1, 4),
            remote(block.at[0], at(0, 0), sems, 2, 2),
            remote(block.at[1], at(0, 1), sems, 3, 4),
            remote(at(2, 0), at(2, 0), sems, 4, 2),
            remote(at(1, 1), at(1, 1), sems, 5, 4),
        ]
        self.own = [pltpu.make_async_copy(block, held, local.at[0]), pltpu.make_async_copy(held, full.at[pl.ds(chip * 2, 2)], local.at[1])]

    def begin(self):
        for copy in (*self.copies[:2], self.own[0]):
            copy.start()

    def more(self):
        for copy in self.copies[2:4]:
            copy.start()

    def middle(self):
        self.own[0].wait()
        self.own[1].start()
        self.copies[1].wait_recv()
        self.copies[4].start()
        self.copies[0].wait_recv()
        self.copies[5].start()

    def late(self):
        pass

    def end(self):
        for n in (2, 3, 4, 5):
            self.copies[n].wait_recv()

    def finish(self):
        pass

    def close(self):
        for copy in self.copies:
            copy.wait_send()
        self.own[1].wait()


class Scatter:
    bits = (1, 2, 4)

    def __init__(self, blocks, rows):
        _, r, n = blocks.shape
        self.ins, self.rows = [blocks], rows
        self.outs = [jax.ShapeDtypeStruct((r, n), BF16)] * 2 if rows else [jax.ShapeDtypeStruct((2, r, n), BF16)]
        self.scratch = [pltpu.VMEM((2, r, n), BF16)] * 6 + [pltpu.SemaphoreType.DMA((4,))] + [pltpu.SemaphoreType.DMA((7,))] * 2

    def bind(self, ins, outs, scratch, own):
        (blocks,), (came, mine, total, by_y, by_x, held, local, *sems) = ins, scratch
        core, chip = lax.axis_index("dp") % 2, lax.axis_index("dp") // 2
        at = lambda bit, half: blocks.at[other(chip, bit) * 2 + half]
        diagonal = lambda half: blocks.at[(3 - chip) * 2 + half]
        self.came, self.mine, self.total, self.by_y, self.by_x, self.held = came, mine, total, by_y, by_x, held
        self.copies = [
            remote(diagonal(0), came.at[0], sems, 0, 4),
            remote(diagonal(1), came.at[1], sems, 1, 2),
            remote(at(2, 0), by_x.at[0], sems, 2, 4),
            remote(at(1, 1), by_y.at[1], sems, 3, 2),
            remote(total.at[0], by_y.at[0], sems, 4, 2),
            remote(total.at[1], by_x.at[1], sems, 5, 4),
        ]
        self.own = [pltpu.make_async_copy(at(1, 0), mine.at[0], local.at[0]), pltpu.make_async_copy(at(2, 1), mine.at[1], local.at[1])]
        self.own += [pltpu.make_async_copy(blocks.at[pl.ds(chip * 2, 2)], held, local.at[2])]
        if self.rows:
            self.out = pltpu.make_async_copy(held.at[core], outs[0], local.at[3])
            self.tell = remote(held.at[1 - core], outs[1], sems, 6, 1)
        else:
            self.out = pltpu.make_async_copy(held, outs[0], local.at[3])

    def begin(self):
        for copy in (*self.copies[:2], *self.own):
            copy.start()

    def more(self):
        for copy in self.copies[2:4]:
            copy.start()

    def middle(self):
        for half in range(2):
            self.copies[half].wait_recv()
            self.own[half].wait()
            self.total[half] = (self.came[half].astype(F32) + self.mine[half].astype(F32)).astype(BF16)

    def late(self):
        self.copies[4].start()
        self.copies[5].start()

    def end(self):
        for n in (2, 3, 4, 5):
            self.copies[n].wait_recv()
        self.own[2].wait()
        self.held[...] = (self.held[...].astype(F32) + self.by_y[...].astype(F32) + self.by_x[...].astype(F32)).astype(BF16)

    def finish(self):
        self.out.start()
        if self.rows:
            self.tell.start()

    def close(self):
        for copy in self.copies:
            copy.wait_send()
        self.out.wait()
        if self.rows:
            self.tell.wait()


def run(name, cid, compute, grid, ins, in_specs, outs, out_specs, scratch=(), comms=(), bits=(), when=(0.4, 0.5), flops=0, start=0, resident=(), closing=None):
    steps = math.prod(grid)
    bits = sorted(set(bits).union(*(comm.bits for comm in comms)))
    middle, late = (min(steps - 1, int(steps * w)) for w in when)
    if not bits:
        for a, i in resident:
            shape = a.shape if i is None else (a.shape[0], None, *a.shape[2:])
            place = (0,) * a.ndim if i is None else (0, i) + (0,) * (a.ndim - 2)
            ins, in_specs = [*ins, a], [*in_specs, pl.BlockSpec(shape, lambda *_, place=place: place, pipeline_mode=pl.Buffered(1))]
        resident = ()
    ins, in_specs, scratch = list(ins) + [a for a, _ in resident], list(in_specs) + [ANY] * len(resident), list(scratch)
    parts_of = [jax.eval_shape(lambda a, i=i: a if i is None else a[:, i], a) for a, i in resident]
    scratch += [pltpu.VMEM(a.shape, a.dtype) for a in parts_of] + [pltpu.SemaphoreType.DMA((len(resident),))] * bool(resident)
    counts = [len(ins)] + [len(c.ins) for c in comms] + [len(outs)] + [len(c.outs) for c in comms] + [len(scratch)] + [len(c.scratch) for c in comms]

    def kernel(*refs):
        refs, groups = list(refs), []
        for count in counts:
            groups.append(refs[:count])
            refs = refs[count:]
        step = 0
        for axis, size in enumerate(grid):
            step = step * size + pl.program_id(axis)
        k = len(comms) + 1
        held = len(resident)
        own = groups[0], groups[k], groups[2 * k]
        if held:
            here, own_scratch, sems = own[2][-held - 1 : -1], own[2][: -held - 1], own[2][-1]
            sources = own[0][-held:]
            own = own[0][:-held] + here, own[1], own_scratch

        def bring():
            for n, (_, i) in enumerate(resident):
                yield pltpu.make_async_copy(sources[n] if i is None else sources[n].at[:, i], here[n], sems.at[n])

        def do(*names):
            for n, comm in enumerate(comms):
                comm.bind(groups[1 + n], groups[k + 1 + n], groups[2 * k + 1 + n], own)
            for what in names:
                if what == "end":
                    for comm, before in zip([*comms, None], [None, *comms], strict=True):
                        if comm:
                            comm.end()
                        if before:
                            before.finish()
                    continue
                for comm in comms:
                    getattr(comm, what)()

        @pl.when(step == 0)
        def _():
            for copy in bring():
                copy.start()
            if bits:
                barrier = pltpu.get_barrier_semaphore()
                for bit in bits:
                    pl.semaphore_signal(barrier, inc=1, device_id={"dp": other(lax.axis_index("dp"), bit)}, device_id_type=MESH)
                pl.semaphore_wait(barrier, len(bits))
            if not start:
                do("begin", "more")
            for copy in bring():
                copy.wait()

        compute(*own)
        for at, what in ((start, ("begin", "more")), (middle, ("middle",)), (late, ("late",)), (steps - 1, ("end", "close"))):
            if comms and (start or at or what[0] != "begin"):

                @pl.when(step == at)
                def _():
                    do(*what)

        if closing:

            @pl.when(step == steps - 1)
            def _():
                closing(*own)

    params = dict(collective_id=cid, has_side_effects=True) if bits else {}
    results = pl.pallas_call(
        kernel,
        name=name,
        grid=grid,
        in_specs=list(in_specs) + [ANY for c in comms for _ in c.ins],
        out_specs=list(out_specs) + [ANY for c in comms for _ in c.outs],
        out_shape=list(outs) + [o for c in comms for o in c.outs],
        scratch_shapes=list(scratch) + [s for c in comms for s in c.scratch],
        compiler_params=pltpu.CompilerParams(dimension_semantics=("arbitrary",) * len(grid), vmem_limit_bytes=62 * 2**20, **params),
        cost_estimate=pl.CostEstimate(flops=int(flops), bytes_accessed=0, transcendentals=0),
    )(*ins, *[a for c in comms for a in c.ins])
    results, got = results[: len(outs)], list(results[len(outs) :])
    return results, [[got.pop(0) for _ in comm.outs] for comm in comms]


def solution(mesh):
    size = mesh.shape["dp"]
    chips = size // 2

    def step(x, dy, *arrays):
        weights, m, v = (arrays[i : i + 3] for i in (0, 3, 6))
        layers, rows, ff = weights[0].shape
        d = rows * size
        half = ff // 2
        part = half // PARTS
        share = part // chips
        tokens = x.shape[1]
        every = 2 * tokens
        unit = 2 * every * d * half

        segments = lambda core: [(c * 2 * PARTS * share + core * PARTS * share + p * share, p * part + c * share) for p in range(PARTS) for c in range(chips)]

        cid = iter(range(100))
        wide = every // 4
        col, row = lambda n: pl.BlockSpec((wide, n), lambda j, i: (i, 0)), pl.BlockSpec((wide, part), lambda j, i: (i, j))
        weight = pl.BlockSpec((d, part), lambda j, i: (0, j))
        f32_rows, bf16_rows = jax.ShapeDtypeStruct((every, half), F32), jax.ShapeDtypeStruct((every, half), BF16)

        def gate_of(a, w, fetch):
            def compute(ins, outs, _):
                outs[0][...] = mm(ins[0][...], ins[1][...])

            (gate,), ((got,),) = run("gate", next(cid), compute, (PARTS, 4), [a, w], [col(d), weight], [f32_rows], [row], comms=[fetch], flops=unit)
            return gate, got

        def up_of(a, w, gate, fetch):
            def compute(ins, outs, _):
                up, gate = mm(ins[0][...], ins[2][...]), ins[1][...]
                outs[0][...] = up
                outs[1][...] = (jax.nn.silu(gate) * up).astype(BF16)

            tile = lambda n: pl.BlockSpec((TILE, n), lambda t: (t, 0))
            (up, hidden), ((got,),) = run(
                "up",
                next(cid),
                compute,
                (every // TILE,),
                [a, gate],
                [tile(d), tile(half)],
                [f32_rows, bf16_rows],
                [tile(half)] * 2,
                comms=[fetch],
                flops=unit,
                resident=[(w, None)],
            )
            return up, hidden, got

        def over_cores(name, terms, lhs, lhs_specs, rhs, given, finish, keep, comms):
            tiles = tokens // TILE
            here = pl.BlockSpec((TILE, d), lambda t: (jnp.maximum(t - tiles, 0), 0))

            def compute(ins, outs, scratch):
                sent, came, state, ssem, rsem, ssem2, rsem2, local = scratch
                t = pl.program_id(0)
                product = lambda: terms(ins[: len(lhs)], ins[len(lhs) + len(given) :])
                away = lambda n: remote(sent.at[n], came.at[n], (ssem, rsem), n, 1)
                shared = outs[-1]
                rows_of = lambda n: pl.ds(pl.multiple_of(n * TILE, TILE), TILE)
                tell = lambda n: remote(state.at[n], shared.at[1, rows_of(n)], (ssem2, rsem2), n, 1)
                save = lambda n: pltpu.make_async_copy(state.at[n], shared.at[0, rows_of(n)], local.at[n])
                n = t - tiles

                @pl.when((t > 0) & (t <= tiles))
                def _():
                    away(t - 1).start()

                @pl.when(n > 0)
                def _():
                    tell(n - 1).start()
                    save(n - 1).start()

                @pl.when(t < tiles)
                def _():
                    sent[t] = product()

                @pl.when(n >= 0)
                def _():
                    away(n).wait_recv()
                    results = finish(product() + came[n], *[g[...] for g in ins[len(lhs) : len(lhs) + len(given)]])
                    for out, result in zip(outs[:-1], results[:-1], strict=True):
                        out[...] = result
                    state[n] = results[-1]

                @pl.when(n == tiles - 1)
                def _():
                    tell(tiles - 1).start()
                    save(tiles - 1).start()
                    for n in range(tiles):
                        away(n).wait_send()
                        tell(n).wait()
                        save(n).wait()

            scratch = [pltpu.VMEM((tiles, TILE, d), F32)] * 2 + [pltpu.VMEM((tiles, TILE, d), BF16)] + [pltpu.SemaphoreType.DMA((tiles,))] * 5
            results, got = run(
                name,
                next(cid),
                compute,
                (2 * tiles,),
                [*lhs, *given],
                list(lhs_specs) + [here] * len(given),
                [jax.ShapeDtypeStruct((tokens, d), BF16)] * keep + [jax.ShapeDtypeStruct((2, tokens, d), BF16)],
                [here] * keep + [ANY],
                scratch,
                comms=comms,
                bits=(1,),
                flops=unit,
                resident=[(a, None) for a in rhs],
            )
            return [*results[:-1], results[-1].reshape(every, d)], got

        swapped = lambda n: pl.BlockSpec((TILE, n), lambda t: ((t + tokens // TILE) % (every // TILE), 0))

        def down_of(hidden, w, h, fetches):
            def terms(lhs, rhs):
                return sum(mm(lhs[0][:, p * part : (p + 1) * part], rhs[0][:, p].reshape(part, d)) for p in range(PARTS))

            def finish(total, h):
                h = h + total.astype(BF16)
                return h, normed(h)

            (h, a), got = over_cores("down", terms, [hidden], [swapped(half)], [w.reshape(chips, PARTS, share, d)], [h], finish, 1, fetches)
            return h, a, got

        def by_hidden(by_h, a, given, given_specs, resident, start, keep, comms=()):
            n_steps = every // TILE

            def written(outs, scratch):
                return [pltpu.make_async_copy(scratch[3 + i], outs[i], scratch[6].at[i]) for i in range(3)]

            def closing(ins, outs, scratch):
                for copy in written(outs, scratch):
                    copy.wait()

            def compute(ins, outs, scratch):
                t = pl.program_id(0)

                @pl.when(t == 0)
                def _():
                    for acc in scratch[:3]:
                        acc[...] = jnp.zeros_like(acc)

                by_h, a = ins[0][...], ins[1][...]
                gate, up, by = start(by_h, a, *[r[...] for r in ins[2:]])
                sig = 1 / (1 + jnp.exp(-gate))
                act = gate * sig
                by_up = (by * act).astype(BF16)
                by_gate = (by * up * (sig * (1 + gate * (1 - sig)))).astype(BF16)
                hidden = (act * up).astype(BF16)
                if keep:
                    outs[3][...], outs[4][...] = by_gate, by_up
                for acc, lhs, rhs in zip(scratch[:3], (a, a, hidden), (by_gate, by_up, by_h), strict=True):
                    acc[...] += t_mm(lhs, rhs)

                @pl.when(t == n_steps - 1)
                def _():
                    for i in range(3):
                        scratch[3 + i][...] = scratch[i][...].astype(BF16)
                    for copy in written(outs, scratch):
                        copy.start()

            tile = lambda n: pl.BlockSpec((TILE, n), lambda t: (t, 0))
            outs = [jax.ShapeDtypeStruct((d, part), BF16)] * 2 + [jax.ShapeDtypeStruct((part, d), BF16)]
            out_specs = [ANY] * 3
            if keep:
                outs += [jax.ShapeDtypeStruct((every, part), BF16)] * 2
                out_specs += [tile(part)] * 2
            return run(
                "by_hidden",
                next(cid),
                compute,
                (n_steps,),
                [by_h, a, *given],
                [tile(d), tile(d), *given_specs],
                outs,
                out_specs,
                [pltpu.VMEM(s, t) for t in (F32, BF16) for s in ((d, part), (d, part), (part, d))] + [pltpu.SemaphoreType.DMA((3,))],
                closing=closing,
                comms=comms,
                flops=(6 if keep else 4) * unit // PARTS,
                resident=resident,
            )

        def by_last(by_h, a, wg, wu, wd, comms):
            def start(by_h, a, wg, wu, wd):
                return mm(a, wg), mm(a, wu), mm_t(by_h, wd).astype(BF16).astype(F32)

            return by_hidden(by_h, a, [], [], [(wg, None), (wu, None), (wd, None)], start, True, comms)

        def by_first(p, by_h, a, gate, up, wd, comms):
            def start(by_h, a, gate, up, wd):
                return gate, up, mm_t(by_h, wd.reshape(part, d)).astype(BF16).astype(F32)

            piece = pl.BlockSpec((TILE, part), lambda t: (t, p))
            return by_hidden(by_h, a, [gate, up], [piece, piece], [(wd.reshape(chips, PARTS, share, d), p)], start, False, comms)

        def by_input(by_gates, by_ups, wg, wu, h, by_h, comms=()):
            def terms(lhs, rhs):
                return sum(
                    mm_t(each[...], w[...]) for each, w in zip(lhs, rhs, strict=True)
                )

            def finish(total, h, by_h):
                return (by_h + by_normed(h, total.astype(BF16)),)

            lhs = [*by_gates, *by_ups]
            (by_hs,), got = over_cores("by_input", terms, lhs, [swapped(part)] * len(lhs), [*wg, *wu], [h, by_h], finish, 0, comms)
            return by_hs, got

        def opened(x, dy, w_gate, w_up):
            tiles = tokens // TILE
            count = 2 * layers

            def compute(ins, outs, scratch):
                mine, give, normal, by, ssem, rsem, local, ssem2, rsem2, local2 = scratch
                *blocks, a, dys = outs
                s = pl.program_id(0)
                core = lax.axis_index("dp") % 2
                moved = lambda n: (n,) if n < 2 else range(2 + (n - 2) * PARTS, 2 + (n - 1) * PARTS)
                pieces = lambda ref, m: ref.at[m] if m < 2 else ref.at[2 + (m - 2) // PARTS, :, pl.ds((m - 2) % PARTS * part, part)]
                keep = lambda m: pltpu.make_async_copy(pieces(mine, m), blocks[m].at[core], local.at[m])
                pass_on = lambda m: remote(pieces(give, m), blocks[m].at[core], (ssem, rsem), m, 1)
                rows_of = lambda n: pl.ds(n * TILE, TILE)
                shared = lambda n: [
                    each
                    for i, (state, out) in enumerate(((normal, a), (by, dys)))
                    for each in (
                        remote(state.at[n], out.at[1, rows_of(n)], (ssem2.at[i], rsem2.at[i]), n, 1),
                        pltpu.make_async_copy(state.at[n], out.at[0, rows_of(n)], local2.at[i, n]),
                    )
                ]
                for n in range(count):
                    for k in range(2):

                        @pl.when((s == n) & (core == k))
                        def _():
                            w = ins[2 + n % 2]
                            for which, half_of in ((mine, k), (give, 1 - k)):
                                for at, to in segments(half_of):
                                    which[n, :, to : to + share] = w[0, :, at : at + share]

                    @pl.when(s == n + 1)
                    def _():
                        for m in moved(n):
                            keep(m).start()
                            pass_on(m).start()

                @pl.when(s == 1)
                def _():
                    keep(0).wait()
                    pass_on(0).wait_recv()

                for n in range(tiles):

                    @pl.when(s == count + n)
                    def _():
                        normal[n] = normed(ins[0][...])
                        by[n] = ins[1][...]

                    @pl.when(s == count + n + 1)
                    def _():
                        for copy in shared(n):
                            copy.start()

                @pl.when(s == count + tiles)
                def _():
                    pass_on(0).wait_send()
                    for m in range(1, len(blocks)):
                        keep(m).wait()
                        pass_on(m).wait()
                    for n in range(tiles):
                        for copy in shared(n):
                            copy.wait()

            tile = pl.BlockSpec((TILE, d), lambda s: (jnp.clip(s - count, 0, tiles - 1), 0))
            matrix = pl.BlockSpec((1, rows, ff), lambda s: (jnp.minimum(s // 2, layers - 1), 0, 0))
            sem = pltpu.SemaphoreType.DMA
            state = jax.ShapeDtypeStruct((2, tokens, d), BF16)
            made = [jax.ShapeDtypeStruct((2, rows, half), BF16)] * 2 + [jax.ShapeDtypeStruct((2, rows, part), BF16)] * ((count - 2) * PARTS)
            (*blocks, a, dys), ((got,),) = run(
                "open",
                next(cid),
                compute,
                (count + tiles + 1,),
                [x, dy, w_gate, w_up],
                [tile, tile, matrix, matrix],
                [*made, state, state],
                [ANY] * (len(made) + 2),
                [pltpu.VMEM((count, rows, half), BF16)] * 2
                + [pltpu.VMEM((tiles, TILE, d), BF16)] * 2
                + [sem((len(made),))] * 3
                + [sem((2, tiles))] * 3,
                comms=[Gather(jax.ShapeDtypeStruct((2, rows, half), BF16), lambda own: own[1][0])],
                bits=(1,),
                when=(0.999, 0.999),
                start=1,
            )
            return blocks, a.reshape(every, d), dys.reshape(every, d), got

        def updated(pieces):
            tile = rows // PARTS
            keys = [(n, p) for n in range(layers) for p in range(PARTS)]

            def kernel(*refs):
                state, refs = refs[:9], refs[9:]
                given, refs = refs[: 5 * len(keys)], refs[5 * len(keys) :]
                outs, scratch = refs[:9], refs[9:]
                core, layer, t = lax.axis_index("dp") % 2, pl.program_id(0), pl.program_id(1)
                for i, key in enumerate(keys):
                    gate_up, down = given[5 * i : 5 * i + 4], given[5 * i + 4]
                    for k in range(2):

                        @pl.when((core == k) & (layer == key[0]))
                        def _():
                            for which, source in enumerate(gate_up):
                                for at, to in segments(k if which % 2 == 0 else 1 - k):
                                    if to // part == key[1]:
                                        scratch[which // 2][:, at : at + share] = source[:, to % part : to % part + share].astype(F32)

                    @pl.when((layer == key[0]) & (t == key[1]))
                    def _():
                        scratch[2][...] = down[...].reshape(scratch[2].shape).astype(F32)

                for i in range(3):
                    w, m, v = (state[i + 3 * j][0] for j in range(3))
                    outs[i][0], outs[i + 3][0], outs[i + 6][0] = adamw(w.astype(F32), m, v, scratch[i][...])

            block = lambda a: pl.BlockSpec((1, a.shape[1] // PARTS, a.shape[2]), lambda n, t: (n, t, 0))
            given, given_specs = [], []
            for n, p in keys:
                given += pieces[n, p]
                given_specs += [pl.BlockSpec((tile, part), lambda k, t, n=n: (jnp.where(k == n, t, 0), 0))] * 4
                given_specs += [pl.BlockSpec(pieces[n, p][4].shape, lambda k, t: (0, 0, 0), pipeline_mode=pl.Buffered(1))]
            wide = lambda a, dtype: jax.ShapeDtypeStruct(a.shape, dtype)
            return pl.pallas_call(
                kernel,
                name="adamw",
                grid=(layers, PARTS),
                in_specs=[block(a) for a in (*weights, *m, *v)] + given_specs,
                out_specs=[block(a) for a in (*weights, *m, *v)],
                out_shape=[wide(a, BF16) for a in weights] + [wide(a, F32) for a in (*m, *v)],
                scratch_shapes=[pltpu.VMEM((a.shape[1] // PARTS, a.shape[2]), F32) for a in weights],
                compiler_params=pltpu.CompilerParams(dimension_semantics=("arbitrary",) * 2, vmem_limit_bytes=62 * 2**20),
            )(*weights, *m, *v, *given)

        flat = lambda w: w.reshape(-1, w.shape[-1])
        h0 = x[0]
        down_all = Gather(weights[2].reshape(layers, 2, -1, d), index=0)
        down_part = lambda p: Gather(weights[2].reshape(layers, PARTS, 2, -1, d), index=(1, p))
        (_, up_block, *parts), a0, dys, wg0 = opened(h0, dy[0], weights[0], weights[1])
        fetch = [[Gather(parts[p]), Gather(parts[PARTS + p]), down_part(p)] for p in range(PARTS)]
        gate0, wu0 = gate_of(a0, flat(wg0), Gather(up_block))
        up0, hidden0, wd0 = up_of(a0, flat(wu0), gate0, down_all)
        h1, a1, got = down_of(hidden0, wd0, h0, fetch[0])

        def scatters(made):
            return [Scatter(g.reshape(8, -1, g.shape[-1]), i < 2) for i, g in enumerate(made[:3])]

        full = [[flat(w) for (w,) in got]]
        made, sums = [], []
        for p in range(PARTS):
            beside = [[*fetch[1], fetch[2][0]], fetch[2][1:], []][p]
            send = [c for each in made for c in scatters(each)][[0, 0, 2][p] : [0, 2, 6][p]]
            results, got = by_last(dys, a1, *full[p], [*beside, *send])
            made.append(results)
            got_w, got_g = [flat(w) for (w,) in got[: len(beside)]], got[len(beside) :]
            sums += got_g
            if p == 0:
                full += [got_w[:3], got_w[3:]]
            if p == 1:
                full[2] += got_w
        columns = list(zip(*full, strict=True))
        by_hs, got = by_input([r[3] for r in made], [r[4] for r in made], columns[0], columns[1], h1, dy[0], scatters(made[2]))
        sums += got
        mine = {(1, p): sum(sums[3 * p : 3 * p + 3], []) for p in range(PARTS)}
        results = None
        for p in range(PARTS):
            results, got = by_first(p, by_hs, a0, gate0, up0, wd0, scatters(results) if p else [])
            if p:
                mine[0, p - 1] = sum(got, [])
        mine[0, PARTS - 1] = sum(run("last", next(cid), lambda *_: None, (1,), [], [], [], [], comms=scatters(results))[1], [])
        return tuple(updated(mine))

    states, cut = P(("rep", "dp"), None, None), P(None, "dp", None)
    return jax.shard_map(
        step,
        mesh=mesh,
        in_specs=(states, states) + (cut,) * 9,
        out_specs=(P("rep", "dp", None),) * 9,
        check_vma=False,
    )
```

```python
import functools
import math

import jax
import jax.numpy as jnp
from jax import lax
from jax.experimental import pallas as pl
from jax.experimental.pallas import tpu as pltpu
from jax.sharding import PartitionSpec as P

F32, BF16 = jnp.float32, jnp.bfloat16
MESH = pl.DeviceIdType.MESH
ANY = pl.BlockSpec(memory_space=pl.ANY)
PARTS = 3
TILE = 512
CORE, Y, X = 1, 2, 4
HERE, LOW, HIGH = 0, 0, 1


def mm(a, w):
    return lax.dot_general(a, w, (((1,), (0,)), ((), ())), preferred_element_type=F32)


def mm_t(a, w):
    return lax.dot_general(a, w, (((1,), (1,)), ((), ())), preferred_element_type=F32)


def t_mm(a, d):
    return lax.dot_general(a, d, (((0,), (0,)), ((), ())), preferred_element_type=F32)


def normed(h):
    wide = h.astype(F32)
    scale = lax.rsqrt(jnp.mean(wide**2, -1, keepdims=True) + 1e-6)
    return (wide * scale).astype(BF16)


def by_normed(h, by_a):
    wide, by = h.astype(F32), by_a.astype(F32)
    scale = lax.rsqrt(jnp.mean(wide**2, -1, keepdims=True) + 1e-6)
    return (scale * by - wide * (scale**3 * jnp.mean(wide * by, -1, keepdims=True))).astype(BF16)


def adamw(w, m, v, g):
    m = 0.9 * m + 0.1 * g
    v = 0.95 * v + 0.05 * g * g
    step = m * lax.rsqrt(v + 1e-8) + 0.1 * w
    return (w - 0.02 * step).astype(BF16), m, v


def other(me, bit):
    return me + bit - 2 * bit * ((me // bit) % 2)


def remote(src, dst, sems, n, bit):
    return pltpu.make_async_remote_copy(
        src_ref=src,
        dst_ref=dst,
        send_sem=sems[0].at[n],
        recv_sem=sems[1].at[n],
        device_id={"dp": other(lax.axis_index("dp"), bit)},
        device_id_type=MESH,
    )


class Gather:
    bits = (Y, X)

    def __init__(self, block, source=None, index=None):
        _, r, n = block.shape[-3:]
        self.source = source
        self.index = index
        self.ins = [] if source else [block]
        self.outs = [jax.ShapeDtypeStruct((8, r, n), block.dtype)]
        self.scratch = [pltpu.VMEM((2, r, n), block.dtype), pltpu.SemaphoreType.DMA((2,)), pltpu.SemaphoreType.DMA((6,)), pltpu.SemaphoreType.DMA((6,))]

    def bind(self, ins, outs, scratch, own):
        (full,), (held, local, *sems) = outs, scratch
        block = self.source(own) if self.source else ins[0] if self.index is None else ins[0].at[self.index]
        chip = lax.axis_index("dp") // 2
        at = lambda bit, half: full.at[other(chip, bit) * 2 + half] if bit else full.at[chip * 2 + half]
        moves = [(block.at[half], at(HERE, half), bit) for half, bit in ((HIGH, Y), (LOW, X), (LOW, Y), (HIGH, X))]
        moves += [(at(*near), at(*near), bit) for near, bit in (((X // 2, LOW), Y), ((Y // 2, HIGH), X))]
        self.copies = [remote(source, to, sems, n, bit) for n, (source, to, bit) in enumerate(moves)]
        self.own = [pltpu.make_async_copy(block, held, local.at[0]), pltpu.make_async_copy(held, full.at[pl.ds(chip * 2, 2)], local.at[1])]

    def begin(self):
        for copy in (*self.copies[:2], self.own[0]):
            copy.start()

    def more(self):
        for copy in self.copies[2:4]:
            copy.start()

    def middle(self):
        self.own[0].wait()
        self.own[1].start()
        self.copies[1].wait_recv()
        self.copies[4].start()
        self.copies[0].wait_recv()
        self.copies[5].start()

    def late(self):
        pass

    def end(self):
        for copy in self.copies[2:]:
            copy.wait_recv()

    def finish(self):
        pass

    def close(self):
        for copy in self.copies:
            copy.wait_send()
        self.own[1].wait()


class Scatter:
    bits = (CORE, Y, X)

    def __init__(self, blocks, rows):
        _, r, n = blocks.shape
        self.ins, self.rows = [blocks], rows
        self.outs = [jax.ShapeDtypeStruct((r, n), BF16)] * 2 if rows else [jax.ShapeDtypeStruct((2, r, n), BF16)]
        self.scratch = [pltpu.VMEM((2, r, n), BF16)] * 6 + [pltpu.SemaphoreType.DMA((4,))] + [pltpu.SemaphoreType.DMA((7,))] * 2

    def bind(self, ins, outs, scratch, own):
        (blocks,), (came, mine, total, by_y, by_x, held, local, *sems) = ins, scratch
        core, chip = lax.axis_index("dp") % 2, lax.axis_index("dp") // 2
        at = lambda bit, half: blocks.at[other(chip, bit) * 2 + half]
        diagonal = lambda half: blocks.at[(3 - chip) * 2 + half]
        self.came, self.mine, self.total, self.by_y, self.by_x, self.held = came, mine, total, by_y, by_x, held
        moves = [(diagonal(half), came.at[half], bit) for half, bit in ((LOW, X), (HIGH, Y))]
        moves += [(at(bit // 2, half), to.at[half], bit) for half, bit, to in ((LOW, X, by_x), (HIGH, Y, by_y))]
        moves += [(total.at[half], to.at[half], bit) for half, bit, to in ((LOW, Y, by_y), (HIGH, X, by_x))]
        self.copies = [remote(source, to, sems, n, bit) for n, (source, to, bit) in enumerate(moves)]
        self.own = [pltpu.make_async_copy(at(bit // 2, half), mine.at[half], local.at[half]) for half, bit in ((LOW, Y), (HIGH, X))]
        self.own += [pltpu.make_async_copy(blocks.at[pl.ds(chip * 2, 2)], held, local.at[2])]
        if self.rows:
            self.out = pltpu.make_async_copy(held.at[core], outs[0], local.at[3])
            self.tell = remote(held.at[1 - core], outs[1], sems, 6, 1)
        else:
            self.out = pltpu.make_async_copy(held, outs[0], local.at[3])

    def begin(self):
        for copy in (*self.copies[:2], *self.own):
            copy.start()

    def more(self):
        for copy in self.copies[2:4]:
            copy.start()

    def middle(self):
        for half in range(2):
            self.copies[half].wait_recv()
            self.own[half].wait()
            self.total[half] = (self.came[half].astype(F32) + self.mine[half].astype(F32)).astype(BF16)

    def late(self):
        self.copies[4].start()
        self.copies[5].start()

    def end(self):
        for copy in self.copies[2:]:
            copy.wait_recv()
        self.own[2].wait()
        self.held[...] = (self.held[...].astype(F32) + self.by_y[...].astype(F32) + self.by_x[...].astype(F32)).astype(BF16)

    def finish(self):
        self.out.start()
        if self.rows:
            self.tell.start()

    def close(self):
        for copy in self.copies:
            copy.wait_send()
        self.out.wait()
        if self.rows:
            self.tell.wait()


def run(name, cid, compute, grid, ins, in_specs, outs, out_specs, scratch=(), comms=(), bits=(), when=(0.4, 0.5), flops=0, start=0, resident=(), closing=None):
    steps = math.prod(grid)
    bits = sorted(set(bits).union(*(comm.bits for comm in comms)))
    middle, late = (min(steps - 1, int(steps * w)) for w in when)
    if not bits:
        for a, i in resident:
            shape = a.shape if i is None else (a.shape[0], None, *a.shape[2:])
            place = (0,) * a.ndim if i is None else (0, i) + (0,) * (a.ndim - 2)
            ins, in_specs = [*ins, a], [*in_specs, pl.BlockSpec(shape, lambda *_, place=place: place, pipeline_mode=pl.Buffered(1))]
        resident = ()
    ins, in_specs, scratch = list(ins) + [a for a, _ in resident], list(in_specs) + [ANY] * len(resident), list(scratch)
    parts_of = [jax.eval_shape(lambda a, i=i: a if i is None else a[:, i], a) for a, i in resident]
    scratch += [pltpu.VMEM(a.shape, a.dtype) for a in parts_of] + [pltpu.SemaphoreType.DMA((len(resident),))] * bool(resident)
    counts = [len(ins)] + [len(c.ins) for c in comms] + [len(outs)] + [len(c.outs) for c in comms] + [len(scratch)] + [len(c.scratch) for c in comms]

    def kernel(*refs):
        refs, groups = list(refs), []
        for count in counts:
            groups.append(refs[:count])
            refs = refs[count:]
        step = 0
        for axis, size in enumerate(grid):
            step = step * size + pl.program_id(axis)
        k = len(comms) + 1
        held = len(resident)
        own = groups[0], groups[k], groups[2 * k]
        if held:
            here, own_scratch, sems = own[2][-held - 1 : -1], own[2][: -held - 1], own[2][-1]
            sources = own[0][-held:]
            own = own[0][:-held] + here, own[1], own_scratch

        def bring():
            for n, (_, i) in enumerate(resident):
                yield pltpu.make_async_copy(sources[n] if i is None else sources[n].at[:, i], here[n], sems.at[n])

        def do(*names):
            for n, comm in enumerate(comms):
                comm.bind(groups[1 + n], groups[k + 1 + n], groups[2 * k + 1 + n], own)
            for what in names:
                if what == "end":
                    for comm, before in zip([*comms, None], [None, *comms], strict=True):
                        if comm:
                            comm.end()
                        if before:
                            before.finish()
                    continue
                for comm in comms:
                    getattr(comm, what)()

        @pl.when(step == 0)
        def _():
            for copy in bring():
                copy.start()
            if bits:
                barrier = pltpu.get_barrier_semaphore()
                for bit in bits:
                    pl.semaphore_signal(barrier, inc=1, device_id={"dp": other(lax.axis_index("dp"), bit)}, device_id_type=MESH)
                pl.semaphore_wait(barrier, len(bits))
            if not start:
                do("begin", "more")
            for copy in bring():
                copy.wait()

        compute(*own)
        for at, what in ((start, ("begin", "more")), (middle, ("middle",)), (late, ("late",)), (steps - 1, ("end", "close"))):
            if comms and (start or at or what[0] != "begin"):

                @pl.when(step == at)
                def _():
                    do(*what)

        if closing:

            @pl.when(step == steps - 1)
            def _():
                closing(*own)

    params = dict(collective_id=cid, has_side_effects=True) if bits else {}
    results = pl.pallas_call(
        kernel,
        name=name,
        grid=grid,
        in_specs=list(in_specs) + [ANY for c in comms for _ in c.ins],
        out_specs=list(out_specs) + [ANY for c in comms for _ in c.outs],
        out_shape=list(outs) + [o for c in comms for o in c.outs],
        scratch_shapes=list(scratch) + [s for c in comms for s in c.scratch],
        compiler_params=pltpu.CompilerParams(dimension_semantics=("arbitrary",) * len(grid), vmem_limit_bytes=62 * 2**20, **params),
        cost_estimate=pl.CostEstimate(flops=int(flops), bytes_accessed=0, transcendentals=0),
    )(*ins, *[a for c in comms for a in c.ins])
    results, got = results[: len(outs)], list(results[len(outs) :])
    return results, [[got.pop(0) for _ in comm.outs] for comm in comms]


def solution(mesh):
    size = mesh.shape["dp"]
    chips = size // 2

    def step(x, dy, *arrays):
        weights, m, v = (arrays[i : i + 3] for i in (0, 3, 6))
        layers, rows, ff = weights[0].shape
        d = rows * size
        half = ff // 2
        part = half // PARTS
        share = part // chips
        tokens = x.shape[1]
        every = 2 * tokens
        unit = 2 * every * d * half

        segments = lambda core: [(c * 2 * PARTS * share + core * PARTS * share + p * share, p * part + c * share) for p in range(PARTS) for c in range(chips)]

        cid = iter(range(100))
        wide = every // 4
        col, row = lambda n: pl.BlockSpec((wide, n), lambda j, i: (i, 0)), pl.BlockSpec((wide, part), lambda j, i: (i, j))
        weight = pl.BlockSpec((d, part), lambda j, i: (0, j))
        f32_rows, bf16_rows = jax.ShapeDtypeStruct((every, half), F32), jax.ShapeDtypeStruct((every, half), BF16)

        def gate_of(a, w, fetch):
            def compute(ins, outs, _):
                outs[0][...] = mm(ins[0][...], ins[1][...])

            (gate,), ((got,),) = run("gate", next(cid), compute, (PARTS, 4), [a, w], [col(d), weight], [f32_rows], [row], comms=[fetch], flops=unit)
            return gate, got

        def up_of(a, w, gate, fetch):
            def compute(ins, outs, _):
                up, gate = mm(ins[0][...], ins[2][...]), ins[1][...]
                outs[0][...] = up
                outs[1][...] = (jax.nn.silu(gate) * up).astype(BF16)

            tile = lambda n: pl.BlockSpec((TILE, n), lambda t: (t, 0))
            (up, hidden), ((got,),) = run(
                "up",
                next(cid),
                compute,
                (every // TILE,),
                [a, gate],
                [tile(d), tile(half)],
                [f32_rows, bf16_rows],
                [tile(half)] * 2,
                comms=[fetch],
                flops=unit,
                resident=[(w, None)],
            )
            return up, hidden, got

        def over_cores(name, terms, lhs, lhs_specs, rhs, given, finish, keep, comms):
            tiles = tokens // TILE
            here = pl.BlockSpec((TILE, d), lambda t: (jnp.maximum(t - tiles, 0), 0))

            def moves(outs, scratch):
                sent, came, state, ssem, rsem, ssem2, rsem2, local = scratch
                rows_of = lambda n: pl.ds(pl.multiple_of(n * TILE, TILE), TILE)
                away = lambda n: remote(sent.at[n], came.at[n], (ssem, rsem), n, CORE)
                tell = lambda n: remote(state.at[n], outs[-1].at[1, rows_of(n)], (ssem2, rsem2), n, CORE)
                save = lambda n: pltpu.make_async_copy(state.at[n], outs[-1].at[0, rows_of(n)], local.at[n])
                return away, tell, save

            def closing(ins, outs, scratch):
                for n in range(tiles):
                    for copy, wait in zip(moves(outs, scratch), ("wait_send", "wait", "wait"), strict=True):
                        getattr(copy(n), wait)()

            def compute(ins, outs, scratch):
                sent, came, state = scratch[:3]
                t = pl.program_id(0)
                product = lambda: terms(ins[: len(lhs)], ins[len(lhs) + len(given) :])
                away, tell, save = moves(outs, scratch)
                n = t - tiles

                @pl.when((t > 0) & (t <= tiles))
                def _():
                    away(t - 1).start()

                @pl.when(n > 0)
                def _():
                    tell(n - 1).start()
                    save(n - 1).start()

                @pl.when(t < tiles)
                def _():
                    sent[t] = product()

                @pl.when(n >= 0)
                def _():
                    away(n).wait_recv()
                    results = finish(product() + came[n], *[g[...] for g in ins[len(lhs) : len(lhs) + len(given)]])
                    for out, result in zip(outs[:-1], results[:-1], strict=True):
                        out[...] = result
                    state[n] = results[-1]

                @pl.when(n == tiles - 1)
                def _():
                    tell(tiles - 1).start()
                    save(tiles - 1).start()

            scratch = [pltpu.VMEM((tiles, TILE, d), F32)] * 2 + [pltpu.VMEM((tiles, TILE, d), BF16)] + [pltpu.SemaphoreType.DMA((tiles,))] * 5
            results, got = run(
                name,
                next(cid),
                compute,
                (2 * tiles,),
                [*lhs, *given],
                list(lhs_specs) + [here] * len(given),
                [jax.ShapeDtypeStruct((tokens, d), BF16)] * keep + [jax.ShapeDtypeStruct((2, tokens, d), BF16)],
                [here] * keep + [ANY],
                scratch,
                comms=comms,
                bits=(1,),
                flops=unit,
                resident=[(a, None) for a in rhs],
                closing=closing,
            )
            return [*results[:-1], results[-1].reshape(every, d)], got

        swapped = lambda n: pl.BlockSpec((TILE, n), lambda t: ((t + tokens // TILE) % (every // TILE), 0))

        def down_of(hidden, w, h, fetches):
            def terms(lhs, rhs):
                return sum(mm(lhs[0][:, p * part : (p + 1) * part], rhs[0][:, p].reshape(part, d)) for p in range(PARTS))

            def finish(total, h):
                h = h + total.astype(BF16)
                return h, normed(h)

            (h, a), got = over_cores("down", terms, [hidden], [swapped(half)], [w.reshape(chips, PARTS, share, d)], [h], finish, 1, fetches)
            return h, a, got

        def by_hidden(by_h, a, given, given_specs, resident, start, keep, comms=()):
            n_steps = every // TILE

            def written(outs, scratch):
                return [pltpu.make_async_copy(scratch[3 + i], outs[i], scratch[6].at[i]) for i in range(3)]

            def closing(ins, outs, scratch):
                for copy in written(outs, scratch):
                    copy.wait()

            def compute(ins, outs, scratch):
                t = pl.program_id(0)

                @pl.when(t == 0)
                def _():
                    for acc in scratch[:3]:
                        acc[...] = jnp.zeros_like(acc)

                by_h, a = ins[0][...], ins[1][...]
                gate, up, by = start(by_h, a, *[r[...] for r in ins[2:]])
                sig = 1 / (1 + jnp.exp(-gate))
                act = gate * sig
                by_up = (by * act).astype(BF16)
                by_gate = (by * up * (sig * (1 + gate * (1 - sig)))).astype(BF16)
                hidden = (act * up).astype(BF16)
                if keep:
                    outs[3][...], outs[4][...] = by_gate, by_up
                for acc, lhs, rhs in zip(scratch[:3], (a, a, hidden), (by_gate, by_up, by_h), strict=True):
                    acc[...] += t_mm(lhs, rhs)

                @pl.when(t == n_steps - 1)
                def _():
                    for i in range(3):
                        scratch[3 + i][...] = scratch[i][...].astype(BF16)
                    for copy in written(outs, scratch):
                        copy.start()

            tile = lambda n: pl.BlockSpec((TILE, n), lambda t: (t, 0))
            outs = [jax.ShapeDtypeStruct((d, part), BF16)] * 2 + [jax.ShapeDtypeStruct((part, d), BF16)]
            out_specs = [ANY] * 3
            if keep:
                outs += [jax.ShapeDtypeStruct((every, part), BF16)] * 2
                out_specs += [tile(part)] * 2
            return run(
                "by_hidden",
                next(cid),
                compute,
                (n_steps,),
                [by_h, a, *given],
                [tile(d), tile(d), *given_specs],
                outs,
                out_specs,
                [pltpu.VMEM(s, t) for t in (F32, BF16) for s in ((d, part), (d, part), (part, d))] + [pltpu.SemaphoreType.DMA((3,))],
                closing=closing,
                comms=comms,
                flops=(6 if keep else 4) * unit // PARTS,
                resident=resident,
            )

        def by_last(by_h, a, wg, wu, wd, comms):
            def start(by_h, a, wg, wu, wd):
                return mm(a, wg), mm(a, wu), mm_t(by_h, wd).astype(BF16).astype(F32)

            return by_hidden(by_h, a, [], [], [(wg, None), (wu, None), (wd, None)], start, True, comms)

        def by_first(p, by_h, a, gate, up, wd, comms):
            def start(by_h, a, gate, up, wd):
                return gate, up, mm_t(by_h, wd.reshape(part, d)).astype(BF16).astype(F32)

            piece = pl.BlockSpec((TILE, part), lambda t: (t, p))
            return by_hidden(by_h, a, [gate, up], [piece, piece], [(wd.reshape(chips, PARTS, share, d), p)], start, False, comms)

        def by_input(by_gates, by_ups, wg, wu, h, by_h, comms=()):
            def terms(lhs, rhs):
                return sum(
                    mm_t(each[...], w[...]) for each, w in zip(lhs, rhs, strict=True)
                )

            def finish(total, h, by_h):
                return (by_h + by_normed(h, total.astype(BF16)),)

            lhs = [*by_gates, *by_ups]
            (by_hs,), got = over_cores("by_input", terms, lhs, [swapped(part)] * len(lhs), [*wg, *wu], [h, by_h], finish, 0, comms)
            return by_hs, got

        def opened(x, dy, w_gate, w_up):
            tiles = tokens // TILE
            count = 2 * layers

            def compute(ins, outs, scratch):
                mine, give, normal, by, ssem, rsem, local, ssem2, rsem2, local2 = scratch
                *blocks, a, dys = outs
                s = pl.program_id(0)
                core = lax.axis_index("dp") % 2
                moved = lambda n: (n,) if n < 2 else range(2 + (n - 2) * PARTS, 2 + (n - 1) * PARTS)
                pieces = lambda ref, m: ref.at[m] if m < 2 else ref.at[2 + (m - 2) // PARTS, :, pl.ds((m - 2) % PARTS * part, part)]
                keep = lambda m: pltpu.make_async_copy(pieces(mine, m), blocks[m].at[core], local.at[m])
                pass_on = lambda m: remote(pieces(give, m), blocks[m].at[core], (ssem, rsem), m, 1)
                rows_of = lambda n: pl.ds(n * TILE, TILE)
                shared = lambda n: [
                    each
                    for i, (state, out) in enumerate(((normal, a), (by, dys)))
                    for each in (
                        remote(state.at[n], out.at[1, rows_of(n)], (ssem2.at[i], rsem2.at[i]), n, 1),
                        pltpu.make_async_copy(state.at[n], out.at[0, rows_of(n)], local2.at[i, n]),
                    )
                ]
                for n in range(count):
                    for k in range(2):

                        @pl.when((s == n) & (core == k))
                        def _():
                            w = ins[2 + n % 2]
                            for which, half_of in ((mine, k), (give, 1 - k)):
                                for at, to in segments(half_of):
                                    which[n, :, to : to + share] = w[0, :, at : at + share]

                    @pl.when(s == n + 1)
                    def _():
                        for m in moved(n):
                            keep(m).start()
                            pass_on(m).start()

                @pl.when(s == 1)
                def _():
                    keep(0).wait()
                    pass_on(0).wait_recv()

                for n in range(tiles):

                    @pl.when(s == count + n)
                    def _():
                        normal[n] = normed(ins[0][...])
                        by[n] = ins[1][...]

                    @pl.when(s == count + n + 1)
                    def _():
                        for copy in shared(n):
                            copy.start()

                @pl.when(s == count + tiles)
                def _():
                    pass_on(0).wait_send()
                    for m in range(1, len(blocks)):
                        keep(m).wait()
                        pass_on(m).wait()
                    for n in range(tiles):
                        for copy in shared(n):
                            copy.wait()

            tile = pl.BlockSpec((TILE, d), lambda s: (jnp.clip(s - count, 0, tiles - 1), 0))
            matrix = pl.BlockSpec((1, rows, ff), lambda s: (jnp.minimum(s // 2, layers - 1), 0, 0))
            sem = pltpu.SemaphoreType.DMA
            state = jax.ShapeDtypeStruct((2, tokens, d), BF16)
            made = [jax.ShapeDtypeStruct((2, rows, half), BF16)] * 2 + [jax.ShapeDtypeStruct((2, rows, part), BF16)] * ((count - 2) * PARTS)
            (*blocks, a, dys), ((got,),) = run(
                "open",
                next(cid),
                compute,
                (count + tiles + 1,),
                [x, dy, w_gate, w_up],
                [tile, tile, matrix, matrix],
                [*made, state, state],
                [ANY] * (len(made) + 2),
                [pltpu.VMEM((count, rows, half), BF16)] * 2
                + [pltpu.VMEM((tiles, TILE, d), BF16)] * 2
                + [sem((len(made),))] * 3
                + [sem((2, tiles))] * 3,
                comms=[Gather(jax.ShapeDtypeStruct((2, rows, half), BF16), lambda own: own[1][0])],
                bits=(1,),
                when=(0.999, 0.999),
                start=1,
            )
            return blocks, a.reshape(every, d), dys.reshape(every, d), got

        def updated(pieces):
            tile = rows // PARTS
            keys = [(n, p) for n in range(layers) for p in range(PARTS)]

            def kernel(*refs):
                state, refs = refs[:9], refs[9:]
                given, refs = refs[: 5 * len(keys)], refs[5 * len(keys) :]
                outs, scratch = refs[:9], refs[9:]
                core, layer, t = lax.axis_index("dp") % 2, pl.program_id(0), pl.program_id(1)
                for i, key in enumerate(keys):
                    gate_up, down = given[5 * i : 5 * i + 4], given[5 * i + 4]
                    for k in range(2):

                        @pl.when((core == k) & (layer == key[0]))
                        def _():
                            for which, source in enumerate(gate_up):
                                for at, to in segments(k if which % 2 == 0 else 1 - k):
                                    if to // part == key[1]:
                                        scratch[which // 2][:, at : at + share] = source[:, to % part : to % part + share].astype(F32)

                    @pl.when((layer == key[0]) & (t == key[1]))
                    def _():
                        scratch[2][...] = down[...].reshape(scratch[2].shape).astype(F32)

                for i in range(3):
                    w, m, v = (state[i + 3 * j][0] for j in range(3))
                    outs[i][0], outs[i + 3][0], outs[i + 6][0] = adamw(w.astype(F32), m, v, scratch[i][...])

            block = lambda a: pl.BlockSpec((1, a.shape[1] // PARTS, a.shape[2]), lambda n, t: (n, t, 0))
            given, given_specs = [], []
            for n, p in keys:
                given += pieces[n, p]
                given_specs += [pl.BlockSpec((tile, part), lambda k, t, n=n: (jnp.where(k == n, t, 0), 0))] * 4
                given_specs += [pl.BlockSpec(pieces[n, p][4].shape, lambda k, t: (0, 0, 0), pipeline_mode=pl.Buffered(1))]
            wide = lambda a, dtype: jax.ShapeDtypeStruct(a.shape, dtype)
            return pl.pallas_call(
                kernel,
                name="adamw",
                grid=(layers, PARTS),
                in_specs=[block(a) for a in (*weights, *m, *v)] + given_specs,
                out_specs=[block(a) for a in (*weights, *m, *v)],
                out_shape=[wide(a, BF16) for a in weights] + [wide(a, F32) for a in (*m, *v)],
                scratch_shapes=[pltpu.VMEM((a.shape[1] // PARTS, a.shape[2]), F32) for a in weights],
                compiler_params=pltpu.CompilerParams(dimension_semantics=("arbitrary",) * 2, vmem_limit_bytes=62 * 2**20),
            )(*weights, *m, *v, *given)

        flat = lambda w: w.reshape(-1, w.shape[-1])
        h0 = x[0]
        down_all = Gather(weights[2].reshape(layers, 2, -1, d), index=0)
        down_part = lambda p: Gather(weights[2].reshape(layers, PARTS, 2, -1, d), index=(1, p))
        (_, up_block, *parts), a0, dys, wg0 = opened(h0, dy[0], weights[0], weights[1])
        fetch = [[Gather(parts[p]), Gather(parts[PARTS + p]), down_part(p)] for p in range(PARTS)]
        gate0, wu0 = gate_of(a0, flat(wg0), Gather(up_block))
        up0, hidden0, wd0 = up_of(a0, flat(wu0), gate0, down_all)
        h1, a1, got = down_of(hidden0, wd0, h0, fetch[0])

        def scatters(made):
            return [Scatter(g.reshape(8, -1, g.shape[-1]), i < 2) for i, g in enumerate(made[:3])]

        full = [[flat(w) for (w,) in got]]
        made, sums = [], []
        for p in range(PARTS):
            beside = [[*fetch[1], fetch[2][0]], fetch[2][1:], []][p]
            send = [c for each in made for c in scatters(each)][[0, 0, 2][p] : [0, 2, 6][p]]
            results, got = by_last(dys, a1, *full[p], [*beside, *send])
            made.append(results)
            got_w, got_g = [flat(w) for (w,) in got[: len(beside)]], got[len(beside) :]
            sums += got_g
            if p == 0:
                full += [got_w[:3], got_w[3:]]
            if p == 1:
                full[2] += got_w
        columns = list(zip(*full, strict=True))
        by_hs, got = by_input([r[3] for r in made], [r[4] for r in made], columns[0], columns[1], h1, dy[0], scatters(made[2]))
        sums += got
        mine = {(1, p): sum(sums[3 * p : 3 * p + 3], []) for p in range(PARTS)}
        results = None
        for p in range(PARTS):
            results, got = by_first(p, by_hs, a0, gate0, up0, wd0, scatters(results) if p else [])
            if p:
                mine[0, p - 1] = sum(got, [])
        mine[0, PARTS - 1] = sum(run("last", next(cid), lambda *_: None, (1,), [], [], [], [], comms=scatters(results))[1], [])
        return tuple(updated(mine))

    states, cut = P(("rep", "dp"), None, None), P(None, "dp", None)
    return jax.shard_map(
        step,
        mesh=mesh,
        in_specs=(states, states) + (cut,) * 9,
        out_specs=(P("rep", "dp", None),) * 9,
        check_vma=False,
    )
```
